32 devices in a mesh: wide: 16 (over z, y, x), narrow: 2 (over core).
Axes of the slice: x: 2, y: 2, z: 4, core: 2. Of those that a mesh axis runs over, the one named last changes fastest.
Arguments:
- tokens: bfloat16 [32768, 768], P(('wide', 'narrow')), may hold values from -6 to 6
- segment: int32 [32, 1024], P(('wide', 'narrow')), may hold values from 0 to 3, as said below
- keep: int32 [32, 1024], P(('wide', 'narrow')), may hold values 0 or 1
- cotangent: bfloat16 [32768, 768], P(('wide', 'narrow')), may hold values from -6 to 6
- gain_one: bfloat16 [768], P('wide'), may hold values from 0.5 to 1.5
- bias_one: bfloat16 [768], P('wide'), may hold values from -3 to 3
- w_query: bfloat16 [768, 768], P(None, 'wide'), may hold values from -0.3125 to 0.3125
- b_query: bfloat16 [768], P('wide'), may hold values from -3 to 3
- w_key: bfloat16 [768, 768], P(None, 'wide'), may hold values from -0.21875 to 0.21875
- w_value: bfloat16 [768, 768], P(None, 'wide'), may hold values from -0.21875 to 0.21875
- b_value: bfloat16 [768], P('wide'), may hold values from -3 to 3
- w_out: bfloat16 [768, 768], P(None, 'wide'), may hold values from -1.75 to 1.75
- b_out: bfloat16 [768], P('wide'), may hold values from -3 to 3
- gain_two: bfloat16 [768], P('wide'), may hold values from 0.5 to 1.5
- bias_two: bfloat16 [768], P('wide'), may hold values from -3 to 3
- w_hidden: bfloat16 [768, 3072], P(None, 'wide'), may hold values from -0.21875 to 0.21875
- b_hidden: bfloat16 [3072], P('wide'), may hold values from -3 to 3
- w_proj: bfloat16 [3072, 768], P(None, 'wide'), may hold values from -0.109375 to 0.109375
- b_proj: bfloat16 [768], P('wide'), may hold values from -3 to 3
Outputs:
- mixed: bfloat16 [32768, 768], P(('wide', 'narrow'))
- grad_tokens: float32 [32768, 768], P(('wide', 'narrow'))
- grad_gain_one: float32 [768], P('wide')
- grad_bias_one: float32 [768], P('wide')
- grad_w_query: float32 [768, 768], P(None, 'wide')
- grad_b_query: float32 [768], P('wide')
- grad_w_key: float32 [768, 768], P(None, 'wide')
- grad_w_value: float32 [768, 768], P(None, 'wide')
- grad_b_value: float32 [768], P('wide')
- grad_w_out: float32 [768, 768], P(None, 'wide')
- grad_b_out: float32 [768], P('wide')
- grad_gain_two: float32 [768], P('wide')
- grad_bias_two: float32 [768], P('wide')
- grad_w_hidden: float32 [768, 3072], P(None, 'wide')
- grad_b_hidden: float32 [3072], P('wide')
- grad_w_proj: float32 [3072, 768], P(None, 'wide')
- grad_b_proj: float32 [768], P('wide')
The draws below stay inside these ranges and needn't reach their ends.
Inputs may be any that keep to these rules, and one draw needn't show every extreme that they name: `segment`: each device's row holds either 4 images of 1024 // 4 slots each, numbered 0 to 3 in order, or one image of all 1024 slots, numbered 0; both kinds occur in every draw.
All inputs are finite; a program needn't handle non-finite values. No bound on the sum of `keep` on one device may be relied on, other than what follows from the above.
Results may differ from the reference program's by a relative error of at most 0.014.
Values may be sent and summed in bfloat16 or wider, within the bound.
A program may use at most 384 MiB of HBM per device.

```python
import jax
import jax.numpy as jnp
from jax import lax

D = 768
HEADS = 16
FF = 3072
HDIM = 48
TOK_DEV = 1024
SEGS = 4
TOKENS = 32768
DEVICES = 32


def draw_segment(key, part):
    first, second, third = jax.random.split(key, 3)
    whole = jax.random.randint(first, (DEVICES,), 0, 57) < 7
    forced = jax.random.randint(second, (), 0, DEVICES)
    other = (forced + 1 + jax.random.randint(third, (), 0, DEVICES - 1)) % DEVICES
    rows = jnp.arange(DEVICES)
    whole = (whole | (rows == forced)) & (rows != other)
    pieces = (jnp.arange(TOK_DEV) // (TOK_DEV // SEGS)).astype(jnp.int32)
    return jnp.where(whole[:, None], jnp.int32(0), pieces[None, :]).astype(jnp.int32)


def set_ends(array, stream_key, smallest, largest):
    longest = array.shape.index(max(array.shape))
    spots = []
    for shift in (0, 1):
        where = [jax.random.randint(jax.random.fold_in(stream_key, axis), (), 0, length) for axis, length in enumerate(array.shape)]
        where[longest] = (where[longest] + shift) % array.shape[longest]
        spots.append(tuple(where))
    return array.at[spots[0]].set(smallest).at[spots[1]].set(largest)


def spiked(array, rng, source, target, parts, factor):
    def block_of(position):
        return (jnp.arange(array.shape[position]) // (array.shape[position] // parts)).reshape((-1,) + (1,) * (array.ndim - 1 - position))

    first = jax.random.permutation(rng, parts)[block_of(target)]
    other_side = (block_of(target) + parts // 2) % parts
    return jnp.where((block_of(source) == first) | (block_of(source) == other_side), factor * array, array)


def level_of(key, extent, cuts, least, high):
    factor_of, own = 1.0, jax.random.fold_in(key, 6)
    for axis_at, parts in cuts:
        steps = jnp.exp(jax.random.uniform(jax.random.fold_in(own, axis_at), (parts,), jnp.float32, least / len(cuts), high / len(cuts)))
        factor_of = factor_of * jnp.repeat(steps, extent[axis_at] // parts).reshape([-1 if axis == axis_at else 1 for axis in range(len(extent))])
    return factor_of


def bell_draw(rng, dims, spread, limit, shards=(), held_as=jnp.bfloat16):
    level = level_of(rng, dims, shards, -0.22, 0.18) if shards else 1.0
    drawn = jax.random.normal(rng, dims, jnp.float32) * spread * level
    return jnp.minimum(jnp.maximum(drawn, -limit), limit).astype(held_as)


def noise_with(own_key, extent, width, most, cuts, heavy, held_as=jnp.bfloat16):
    result = width * jax.random.normal(own_key, extent, jnp.float32)
    if cuts:
        result = result * level_of(own_key, extent, cuts, -0.22, 0.18)
    return jnp.clip(spiked(result, jax.random.fold_in(own_key, 3), *heavy), -most, most).astype(held_as)


def setup_inputs(seed: int = 0) -> dict:
    arg_keys = jax.random.split(jax.random.key(seed), 20)
    tokens = bell_draw(arg_keys[0], (TOKENS, D), 1.0, 6.0, ((0, 32),))
    segment = draw_segment(jax.random.fold_in(arg_keys[19], 71), 0)
    keep = set_ends((jax.random.randint(arg_keys[2], (DEVICES, TOK_DEV), 0, 8) < 7).astype(jnp.int32), jax.random.fold_in(arg_keys[2], 1), 0, 1)
    cotangent = noise_with(arg_keys[3], (TOKENS, D), 1.0, 6.0, ((0, 32),), (0, 1, 32, 2.75))
    gain_one = jnp.clip(1.0 + 0.1 * jax.random.normal(arg_keys[4], (D,), jnp.float32), 0.5, 1.5).astype(jnp.bfloat16)
    bias_one = bell_draw(arg_keys[5], (D,), 0.5, 3.0, ((0, 16),))
    w_query = bell_draw(arg_keys[6], (D, D), (D // 2) ** -0.5, 0.3125, ((1, 16),))
    b_query = bell_draw(arg_keys[7], (D,), 0.5, 3.0, ((0, 16),))
    w_key = bell_draw(arg_keys[8], (D, D), D ** -0.5, 0.21875, ((1, 16),))
    w_value = bell_draw(arg_keys[9], (D, D), D ** -0.5, 0.21875, ((1, 16),))
    b_value = bell_draw(arg_keys[10], (D,), 0.5, 3.0, ((0, 16),))
    w_out = bell_draw(arg_keys[11], (D, D), (D // 64) ** -0.5, 1.75, ((1, 16),))
    b_out = bell_draw(arg_keys[12], (D,), 0.5, 3.0, ((0, 16),))
    gain_two = jnp.clip(1.0 + 0.1 * jax.random.normal(arg_keys[13], (D,), jnp.float32), 0.5, 1.5).astype(jnp.bfloat16)
    bias_two = bell_draw(arg_keys[14], (D,), 0.5, 3.0, ((0, 16),))
    w_hidden = bell_draw(arg_keys[15], (D, FF), D ** -0.5, 0.21875, ((1, 16),))
    b_hidden = bell_draw(arg_keys[16], (FF,), 0.5, 3.0, ((0, 16),))
    w_proj = bell_draw(arg_keys[17], (FF, D), FF ** -0.5, 0.109375, ((1, 16),))
    b_proj = bell_draw(arg_keys[18], (D,), 0.5, 3.0, ((0, 16),))
    return dict(tokens=tokens, segment=segment, keep=keep, cotangent=cotangent, gain_one=gain_one, bias_one=bias_one, w_query=w_query, b_query=b_query, w_key=w_key, w_value=w_value, b_value=b_value, w_out=w_out, b_out=b_out, gain_two=gain_two, bias_two=bias_two, w_hidden=w_hidden, b_hidden=b_hidden, w_proj=w_proj, b_proj=b_proj)


@jax.custom_vjp
def low(v):
    return lax.optimization_barrier(v.astype(jnp.bfloat16)).astype(jnp.float32)

@jax.custom_vjp
def low_back(v):
    return v

def low_keep(v):
    return (low(v), None)

def low_pass(kept, grad):
    return (grad,)

def back_keep(v):
    return (v, None)

def back_low(kept, grad):
    return (low(grad),)
low.defvjp(low_keep, low_pass)
low_back.defvjp(back_keep, back_low)

def mat(a, b):
    return jnp.dot(a, b, precision=lax.Precision.HIGHEST)

def layer_norm_rows(v, gain, bias):
    centred = v - lax.optimization_barrier(jnp.mean(v, -1, keepdims=True))
    var = lax.optimization_barrier(jnp.mean(centred * centred, -1, keepdims=True))
    return centred * lax.rsqrt(var + 1e-05) * gain + bias

def attend_block(block):
    query, key_block, value, seg, live = block
    scale = float(HDIM) ** (-0.5)
    scores = jnp.einsum('qhd,khd->hqk', query, key_block, precision=lax.Precision.HIGHEST) * scale
    scores = low_back(scores)
    index = jnp.arange(seg.shape[0])
    allowed = (seg[:, None] == seg[None, :]) & ((live[None, :] > 0) | (index[:, None] == index[None, :]))
    scores = jnp.where(allowed[None], scores, jnp.float32(-1e+30))
    probs = low(jax.nn.softmax(scores, axis=-1))
    return jnp.einsum('hqk,khd->qhd', probs, value, precision=lax.Precision.HIGHEST)

def reference(tokens, segment, keep, cotangent, gain_one, bias_one, w_query, b_query, w_key, w_value, b_value, w_out, b_out, gain_two, bias_two, w_hidden, b_hidden, w_proj, b_proj):
    blocks = TOKENS // TOK_DEV
    live = keep.astype(jnp.float32).reshape(-1)

    def forward(input_float, g1, be1, wq, bq, wk, wv, bv, wo, bo, g2, be2, w1, b1, w2, b2):
        h1 = low(layer_norm_rows(input_float, g1, be1))
        query = low(low_back(mat(h1, wq) + bq))
        keys = low(low_back(mat(h1, wk)))
        value = low(low_back(mat(h1, wv) + bv))
        shape = (blocks, TOK_DEV, HEADS, HDIM)
        heads = lax.map(jax.checkpoint(attend_block), (query.reshape(shape), keys.reshape(shape), value.reshape(shape), segment, keep))
        joined = low(low_back(heads.reshape(TOKENS, D)))
        x1 = input_float + low_back(mat(joined, wo) + bo)
        h2 = low(layer_norm_rows(x1, g2, be2))
        upper = low_back(mat(h2, w1) + b1)
        act = low(jax.nn.gelu(upper, approximate=False))
        return x1 + low_back(mat(act, w2) + b2)
    inputs = (tokens, gain_one, bias_one, w_query, b_query, w_key, w_value, b_value, w_out, b_out, gain_two, bias_two, w_hidden, b_hidden, w_proj, b_proj)
    out, pull = jax.vjp(forward, *[a.astype(jnp.float32) for a in inputs])
    grads = pull(cotangent.astype(jnp.float32) * live[:, None])
    grad_x, grad_g1, grad_be1, grad_wq, grad_bq, grad_wk, grad_wv, grad_bv, grad_wo, grad_bo, grad_g2, grad_be2, grad_w1, grad_b1, grad_w2, grad_b2 = grads
    return (out.astype(jnp.bfloat16), grad_x, grad_g1, grad_be1, grad_wq, grad_bq, grad_wk, grad_wv, grad_bv, grad_wo, grad_bo, grad_g2, grad_be2, grad_w1, grad_b1, grad_w2, grad_b2)
```

```python
import functools
import math

import jax
import jax.numpy as jnp
from jax import lax
from jax.experimental import pallas as pl
from jax.experimental.pallas import tpu as pltpu
from jax.sharding import PartitionSpec as P

HEADS = 16
F32 = jnp.float32
BF16 = jnp.bfloat16
MESH = pl.DeviceIdType.MESH
LOG2E = math.log2(math.e)
MASKED = -1e30
SPARE = 16
CHUNK = 256


def dims(left, right, a, b):
    return lax.dot_general(left, right, (((a,), (b,)), ((), ())), preferred_element_type=F32)


def chip_axes(chips):
    if chips == 16:
        return ((4, 4), (2, 2), (1, 2))
    return ((1, chips),)


def axis_orders(axes):
    if len(axes) == 3:
        return ((0, 1, 2), (2, 0, 1))
    return (tuple(range(len(axes))),) * 2


def place(me, axis):
    stride, size = axis
    return lax.rem(lax.div(me, stride), size)


def peer(me, axis, step):
    stride, size = axis
    mine = place(me, axis)
    other = lax.rem(mine + step, size)
    return me + (other - mine) * stride


def greet(me, core, axes):
    barrier = pltpu.get_barrier_semaphore()
    count = 1
    pl.semaphore_signal(barrier, 1, device_id=(me, 1 - core), device_id_type=MESH)
    for axis in axes:
        for step in range(1, axis[1]):
            pl.semaphore_signal(
                barrier, 1, device_id=(peer(me, axis, step), core), device_id_type=MESH
            )
            count += 1
    pl.semaphore_wait(barrier, count)


def held_blocks(me, axes, done):
    ids = [me]
    for a in done:
        stride, size = axes[a]
        ids = [i + (v - place(me, axes[a])) * stride for i in ids for v in range(size)]
    return ids


def half(ref, block, c):
    width = ref.shape[-1] // 2
    return ref.at[block, :, pl.ds(c * width, width)]


def flat_half(ref, c):
    width = ref.shape[-1] // 2
    return ref.at[:, pl.ds(c * width, width)]


def gather_plan(ins, outs, sems, me, c, axes):
    order = axis_orders(axes)[c]
    send, recv, pass_send, pass_recv, own = sems
    chips = outs[0].shape[0]
    stages = []
    count = [0]
    passed = [0]
    pending = []

    def hand_over(ids, first=False):
        for n, block in enumerate(ids):
            for k, (src, dst) in enumerate(zip(ins, outs)):
                slot = passed[0] + n * len(outs) + k
                source = flat_half(src, c) if first else half(dst, block, c)
                pltpu.make_async_remote_copy(
                    source, half(dst, block, c), pass_send.at[slot], pass_recv.at[slot],
                    device_id=(me, 1 - c), device_id_type=MESH,
                ).start()
        passed[0] += len(ids) * len(outs)

    def copies(number):
        axis = axes[order[number]]
        ids = held_blocks(me, axes, order[:number])
        base = sum(
            (axes[order[m]][1] - 1) * math.prod(axes[a][1] for a in order[:m]) * len(outs)
            for m in range(number)
        )
        out = []
        slot = base
        for step in range(1, axis[1]):
            target = peer(me, axis, step)
            source = peer(me, axis, axis[1] - step)
            for block in ids:
                for k, (src, dst) in enumerate(zip(ins, outs)):
                    first = number == 0
                    out.append((
                        pltpu.make_async_remote_copy(
                            flat_half(src, c) if first else half(dst, block, c),
                            half(dst, block, c), send.at[slot], recv.at[slot],
                            device_id=(target, c), device_id_type=MESH,
                        ),
                        block + (source - me),
                    ))
                    slot += 1
        return out

    def begin(number):
        for copy, _ in copies(number):
            copy.start()

    def land(number):
        got = copies(number)
        for copy, _ in got:
            copy.wait_recv()
        return [block for _, block in got[:: len(outs)]]

    def first():
        for k, (src, dst) in enumerate(zip(ins, outs)):
            pltpu.make_async_copy(src, dst.at[me], own.at[k]).start()
        begin(0)

    def middle(number):
        def run():
            blocks = land(number)
            if number == 0:
                for k, (src, dst) in enumerate(zip(ins, outs)):
                    pltpu.make_async_copy(src, dst.at[me], own.at[k]).wait()
            if number + 1 < len(order):
                begin(number + 1)
            hand_over(blocks)
        return run

    def last():
        total = (chips - 1) * len(outs)
        for number in range(len(order)):
            for copy, _ in copies(number):
                copy.wait_send()
        for k in range(total):
            dst = outs[k % len(outs)]
            pltpu.make_async_remote_copy(
                half(dst, me, c), half(dst, me, 1 - c), pass_send.at[k], pass_recv.at[k],
                device_id=(me, 1 - c), device_id_type=MESH,
            ).wait()

    stages.append(first)
    for number in range(len(order)):
        stages.append(middle(number))
    stages.append(last)
    return stages


def gather_sems(chips, arrays):
    total = (chips - 1) * arrays
    return [pltpu.SemaphoreType.DMA((total,)) for _ in range(4)] + [
        pltpu.SemaphoreType.DMA((arrays,))
    ]


def gather_kernel(chips, arrays, *refs):
    ins, outs, sems = refs[:arrays], refs[arrays : 2 * arrays], refs[2 * arrays :]
    me, core = lax.axis_index("wide"), lax.axis_index("narrow")
    axes = chip_axes(chips)
    greet(me, core, axes)
    for c in range(2):
        @pl.when(core == c)
        def _():
            for stage in gather_plan(ins, outs, sems, me, c, axes):
                stage()


def gather(arrays, chips, ident):
    vm = pl.BlockSpec(memory_space=pltpu.VMEM)
    return pl.pallas_call(
        functools.partial(gather_kernel, chips, len(arrays)),
        out_shape=[jax.ShapeDtypeStruct((chips,) + a.shape, a.dtype) for a in arrays],
        in_specs=[vm] * len(arrays),
        out_specs=[pl.BlockSpec(memory_space=pl.ANY)] * len(arrays),
        scratch_shapes=gather_sems(chips, len(arrays)),
        compiler_params=pltpu.CompilerParams(collective_id=ident, has_side_effects=True),
    )(*arrays)


def phase_base(axes, order, number, arrays):
    return sum(
        (axes[order[m]][1] - 1) * math.prod(axes[a][1] for a in order[:m]) * arrays
        for m in range(number)
    )


def scatter_plan(ins, outs, accs, halves, landed, results, sems, me, c, axes):
    order = axis_orders(axes)[c]
    send, recv, swap_send, swap_recv, own, out_sem = sems
    arrays = len(ins)

    def swap():
        copies = []
        for k in range(arrays):
            width = ins[k].shape[-1] // 2
            copies.append((
                pltpu.make_async_remote_copy(
                    ins[k].at[:, :, pl.ds((1 - c) * width, width)], halves[k],
                    swap_send.at[k], swap_recv.at[k],
                    device_id=(me, 1 - c), device_id_type=MESH,
                ),
                pltpu.make_async_copy(
                    ins[k].at[:, :, pl.ds(c * width, width)], accs[k], own.at[k]
                ),
            ))
        return copies

    def copies(number):
        axis = axes[order[number]]
        ids = held_blocks(me, axes, order[:number])
        slot = phase_base(axes, order, number, 1)
        out = []
        for step in range(1, axis[1]):
            target = peer(me, axis, step)
            for block in ids:
                for k in range(arrays):
                    n = slot * arrays + k
                    out.append((
                        pltpu.make_async_remote_copy(
                            accs[k].at[block + (target - me)], landed[k].at[slot],
                            send.at[n], recv.at[n],
                            device_id=(target, c), device_id_type=MESH,
                        ),
                        block, k, slot,
                    ))
                slot += 1
        return out

    def begin(number):
        for copy, *_ in copies(number):
            copy.start()

    def first():
        for remote, local in swap():
            remote.start()
            local.start()

    def add_pair():
        for remote, local in swap():
            local.wait()
            remote.wait()
        for k in range(arrays):
            @pl.loop(0, accs[k].shape[0])
            def _(block):
                accs[k][block] = (
                    accs[k][block].astype(F32) + halves[k][block].astype(F32)
                ).astype(BF16)
        begin(len(order) - 1)

    def add(number):
        def run():
            got = copies(number)
            for copy, *_ in got:
                copy.wait()
            groups = {}
            for position, (_, block, k, slot) in enumerate(got):
                ids = math.prod(axes[a][1] for a in order[:number])
                groups.setdefault((position // arrays % ids, k), (block, []))[1].append(slot)
            for (_, k), (block, slots) in groups.items():
                total = accs[k][block].astype(F32)
                for slot in slots:
                    total = total + landed[k][slot].astype(F32)
                if number:
                    accs[k][block] = total.astype(BF16)
                else:
                    width = total.shape[-1]
                    results[k][:, pl.ds(c * width, width)] = total
            if number:
                begin(number - 1)
            else:
                for copy in finals():
                    copy.start()
        return run

    def finals():
        return [
            pltpu.make_async_remote_copy(
                flat_half(results[k], c), flat_half(results[k], c),
                swap_send.at[arrays + k], swap_recv.at[arrays + k],
                device_id=(me, 1 - c), device_id_type=MESH,
            )
            for k in range(arrays)
        ]

    def last():
        outgoing = [pltpu.make_async_copy(results[k], outs[k], out_sem.at[k]) for k in range(arrays)]
        for copy, out in zip(finals(), outgoing):
            copy.wait()
            out.start()
        for out in outgoing:
            out.wait()

    return [first, add_pair] + [add(n) for n in reversed(range(len(order)))] + [last]


def scatter_scratch(arrays):
    chips = arrays[0].shape[0]
    number = len(arrays)
    scratch = []
    for rows in (chips, chips, chips - 1):
        scratch += [pltpu.VMEM((rows, a.shape[1], a.shape[2] // 2), BF16) for a in arrays]
    scratch += [pltpu.VMEM(a.shape[1:], F32) for a in arrays]
    dma = pltpu.SemaphoreType.DMA
    return scratch + [dma(((chips - 1) * number,)) for _ in range(2)] + [
        dma((n,)) for n in (2 * number, 2 * number, number, number)
    ]


def scatter_parts(arrays, refs):
    parts = [refs[n * arrays : (n + 1) * arrays] for n in range(4)]
    return parts, refs[4 * arrays :]


def scatter_kernel(chips, arrays, *refs):
    ins, outs = refs[:arrays], refs[arrays : 2 * arrays]
    parts, sems = scatter_parts(arrays, refs[2 * arrays :])
    me, core = lax.axis_index("wide"), lax.axis_index("narrow")
    axes = chip_axes(chips)
    greet(me, core, axes)
    for c in range(2):
        @pl.when(core == c)
        def _():
            for stage in scatter_plan(ins, outs, *parts, sems, me, c, axes):
                stage()


def scatter(arrays, ident):
    any_space = pl.BlockSpec(memory_space=pl.ANY)
    return pl.pallas_call(
        functools.partial(scatter_kernel, arrays[0].shape[0], len(arrays)),
        out_shape=[jax.ShapeDtypeStruct(a.shape[1:], F32) for a in arrays],
        in_specs=[any_space] * len(arrays),
        out_specs=[any_space] * len(arrays),
        scratch_shapes=scatter_scratch(arrays),
        compiler_params=pltpu.CompilerParams(
            collective_id=ident, has_side_effects=True, vmem_limit_bytes=60 * 2**20
        ),
    )(*arrays)


def forward_head(qkv, mask, out, lse, head_dim):
    count = qkv.shape[-1]
    factor = head_dim**-0.5 * LOG2E
    keys = qkv[0, head_dim : 2 * head_dim, :]
    value = qkv[0, 2 * head_dim : 3 * head_dim + SPARE, :]

    for start in range(0, count, CHUNK):
        part = pl.ds(start, CHUNK)
        raw = dims(keys, qkv[0, :head_dim, part], 0, 0) * factor + mask[:, part].astype(F32)
        top = jnp.max(raw, 0, keepdims=True)
        probs = jnp.exp2(raw - top).astype(BF16)
        both = dims(value, probs, 1, 0)
        total = both[head_dim : head_dim + 1]
        out[0, :, part] = (both[:head_dim] / total).astype(BF16)
        lse[0, :, part] = top + jnp.log2(total)


def backward_head(qkv, mask, out, d_out, lse, grad, d_key, d_value, head_dim):
    count = qkv.shape[-1]
    scale = head_dim**-0.5
    factor = scale * LOG2E
    keys = qkv[0, head_dim : 2 * head_dim, :]
    value = qkv[0, 2 * head_dim : 3 * head_dim, :]

    for start in range(0, count, CHUNK):
        part = pl.ds(start, CHUNK)
        query = qkv[0, :head_dim, part]
        d_part = d_out[0, :, part]
        probs = jnp.exp2(
            dims(keys, query, 0, 0) * factor + (mask[:, part].astype(F32) - lse[0, :, part])
        )
        share = jnp.sum(d_part.astype(F32) * out[0, :, part].astype(F32), 0, keepdims=True)
        d_probs = dims(value, d_part, 0, 0)
        d_scores = (probs * (d_probs - share)).astype(BF16)
        probs_low = probs.astype(BF16)
        grad[0, :head_dim, part] = (dims(keys, d_scores, 1, 0) * scale).astype(BF16)
        more_value = dims(d_part, probs_low, 1, 1)
        more_key = dims(query, d_scores, 1, 1)
        if start == 0:
            d_value[...] = more_value
            d_key[...] = more_key
        else:
            d_value[...] += more_value
            d_key[...] += more_key
    grad[0, head_dim : 2 * head_dim, :] = (d_key[...] * scale).astype(BF16)
    grad[0, 2 * head_dim : 3 * head_dim, :] = d_value[...].astype(BF16)
    grad[0, 3 * head_dim :, :] = jnp.zeros((SPARE, count), BF16)


def head_spec(rows, count):
    return pl.BlockSpec((1, rows, count), lambda h: (h, 0, 0))


def attention(qkv, mask):
    rows, count = qkv.shape[1:]
    head_dim = (rows - SPARE) // 3

    def body(qkv_ref, mask_ref, out, lse):
        forward_head(qkv_ref, mask_ref, out, lse, head_dim)

    return pl.pallas_call(
        body,
        grid=(HEADS,),
        out_shape=[
            jax.ShapeDtypeStruct((HEADS, head_dim, count), BF16),
            jax.ShapeDtypeStruct((HEADS, 1, count), F32),
        ],
        in_specs=[head_spec(rows, count), pl.BlockSpec((count, count), lambda h: (0, 0))],
        out_specs=[head_spec(head_dim, count), head_spec(1, count)],
        compiler_params=pltpu.CompilerParams(vmem_limit_bytes=60 * 2**20),
    )(qkv, mask)


def attention_back(qkv, mask, out, d_out, lse):
    rows, count = qkv.shape[1:]
    head_dim = (rows - SPARE) // 3

    def body(qkv_ref, mask_ref, out_ref, d_out_ref, lse_ref, grad, d_key, d_value):
        backward_head(
            qkv_ref, mask_ref, out_ref, d_out_ref, lse_ref, grad, d_key, d_value, head_dim
        )

    return pl.pallas_call(
        body,
        grid=(HEADS,),
        out_shape=jax.ShapeDtypeStruct((HEADS, rows, count), BF16),
        in_specs=[
            head_spec(rows, count),
            pl.BlockSpec((count, count), lambda h: (0, 0)),
            head_spec(head_dim, count),
            head_spec(head_dim, count),
            head_spec(1, count),
        ],
        out_specs=head_spec(rows, count),
        scratch_shapes=[pltpu.VMEM((head_dim, count), F32)] * 2,
        compiler_params=pltpu.CompilerParams(vmem_limit_bytes=60 * 2**20),
    )(qkv, mask, out, d_out, lse)


def norm(values):
    centred = values - jnp.mean(values, -1, keepdims=True)
    factor = lax.rsqrt(jnp.mean(centred * centred, -1, keepdims=True) + 1e-05)
    return centred * factor, factor


def norm_back(grad, normed, factor, gain):
    scaled = grad * gain
    inner = (
        scaled
        - jnp.mean(scaled, -1, keepdims=True)
        - normed * jnp.mean(scaled * normed, -1, keepdims=True)
    )
    return factor * inner, jnp.sum(grad * normed, 0), jnp.sum(grad, 0)


def gelu_slope(values):
    cdf = 0.5 * (1.0 + lax.erf(values * (1.0 / math.sqrt(2.0))))
    pdf = jnp.exp(-0.5 * values * values) * (1.0 / math.sqrt(2.0 * math.pi))
    return cdf + values * pdf


def row_sums(values):
    return jnp.sum(values.astype(F32), 0)


def widen(vector, width):
    return jnp.pad(vector, (0, width - vector.shape[0]))


def shards(
    chips,
    replicas,
    tokens,
    segment,
    keep,
    cotangent,
    gain_one,
    bias_one,
    w_query,
    b_query,
    w_key,
    w_value,
    b_value,
    w_out,
    b_out,
    gain_two,
    bias_two,
    w_hidden,
    b_hidden,
    w_proj,
    b_proj,
):
    own_copies = chips == HEADS and replicas == 2
    count, width = tokens.shape
    head_dim = width // HEADS
    hidden = w_hidden.shape[1] * chips
    vectors = (gain_one, bias_one, b_query, b_value, b_out, gain_two, bias_two, b_hidden, b_proj)
    packed = jnp.stack([widen(v, width) for v in vectors])
    packed = jnp.pad(packed, ((0, SPARE - len(vectors)), (0, 0)))

    if own_copies:
        first = jnp.concatenate([w_query.T, w_key.T, w_value.T, packed], 0)
        (first,) = gather([first], chips, 0)
        out_t, hidden_t, proj_t = gather([w_out.T, w_hidden.T, w_proj.T], chips, 1)
        joined_t = first
        vector_rows = first[:, 3 * head_dim :, :]
    else:
        whole = [
            lax.all_gather(w.T, "wide", axis=0, tiled=True) for w in (w_query, w_key, w_value)
        ]
        whole = [w.reshape(HEADS, head_dim, width) for w in whole]
        whole.append(jnp.zeros((HEADS, SPARE, width), BF16))
        joined_t = jnp.concatenate(whole, 1)
        vector_rows = lax.all_gather(packed, "wide", axis=0, tiled=False)
        out_t, hidden_t, proj_t = [
            lax.all_gather(w.T, "wide", axis=0, tiled=False) for w in (w_out, w_hidden, w_proj)
        ]
    out_t = out_t.reshape(width, width)
    hidden_t = hidden_t.reshape(hidden, width)
    proj_t = proj_t.reshape(width, hidden)
    joined_t = joined_t.reshape(HEADS * (3 * head_dim + SPARE), width)
    gain_one_f, bias_one_f, b_query_f, b_value_f, b_out_f, gain_two_f, bias_two_f, b_hidden_f, b_proj_f = [
        vector_rows[:, n, : v.shape[0]].reshape(-1).astype(F32) for n, v in enumerate(vectors)
    ]

    live = keep[0]
    seg = segment[0]
    index = jnp.arange(count)
    allowed = (seg[:, None] == seg[None, :]) & (
        (live[:, None] > 0) | (index[:, None] == index[None, :])
    )
    mask = jnp.where(allowed, 0.0, MASKED).astype(BF16)

    x = tokens.astype(F32)
    xhat_one, factor_one = norm(x)
    h_one = (xhat_one * gain_one_f + bias_one_f).astype(BF16)
    block = 3 * head_dim + SPARE
    offsets = jnp.concatenate(
        [
            b_query_f.reshape(HEADS, head_dim),
            jnp.zeros((HEADS, head_dim), F32),
            b_value_f.reshape(HEADS, head_dim),
            jnp.zeros((HEADS, SPARE), F32),
        ],
        1,
    )
    row = jnp.arange(block)[None, :, None]
    qkv = dims(joined_t, h_one, 1, 1).reshape(HEADS, block, count) + offsets[:, :, None]
    qkv = jnp.where(row < 3 * head_dim, qkv, jnp.where(row == 3 * head_dim, 1.0, 0.0)).astype(BF16)
    o_t, lse = attention(qkv, mask)
    o_flat = o_t.reshape(width, count)
    x_one = x + dims(o_flat, out_t, 0, 1) + b_out_f
    xhat_two, factor_two = norm(x_one)
    h_two = (xhat_two * gain_two_f + bias_two_f).astype(BF16)
    upper = dims(h_two, hidden_t, 1, 1) + b_hidden_f
    act = jax.nn.gelu(upper, approximate=False).astype(BF16)
    mixed = (x_one + dims(act, proj_t, 1, 1) + b_proj_f).astype(BF16)

    d_y = cotangent.astype(F32) * live.astype(F32)[:, None]
    d_m = d_y.astype(BF16)
    grad_proj = dims(d_m, act, 0, 0).astype(BF16)
    d_upper = (dims(d_m, proj_t, 1, 0) * gelu_slope(upper)).astype(BF16)
    grad_hidden = dims(d_upper, h_two, 0, 0).astype(BF16)
    d_two, grad_gain_two, grad_bias_two = norm_back(
        dims(d_upper, hidden_t, 1, 0), xhat_two, factor_two, gain_two_f
    )
    d_x_one = d_y + d_two
    d_attn = d_x_one.astype(BF16)
    grad_out = dims(d_attn, o_flat, 0, 1).astype(BF16)
    d_o = dims(out_t, d_attn, 0, 1).astype(BF16).reshape(HEADS, head_dim, count)
    late = [
        g.reshape(chips, -1, g.shape[-1]) for g in (grad_out, grad_hidden, grad_proj)
    ]
    if own_copies:
        late = scatter(late, 2)
    d_qkv = attention_back(qkv, mask, o_t, d_o, lse)
    d_flat = d_qkv.reshape(HEADS * block, count)
    grad_qkv = dims(d_flat, h_one, 1, 0).reshape(HEADS, block, width)
    bias_sums = jnp.sum(d_qkv.astype(F32), -1)
    d_one, grad_gain_one, grad_bias_one = norm_back(
        dims(d_flat, joined_t, 0, 0), xhat_one, factor_one, gain_one_f
    )
    grad_tokens = d_x_one + d_one

    sums = (
        grad_gain_one,
        grad_bias_one,
        bias_sums[:, :head_dim].reshape(-1),
        bias_sums[:, 2 * head_dim : 3 * head_dim].reshape(-1),
        row_sums(d_attn),
        grad_gain_two,
        grad_bias_two,
        row_sums(d_upper),
        row_sums(d_m),
    )
    sums = jnp.stack(
        [jnp.pad(s.reshape(chips, -1), ((0, 0), (0, width - s.size // chips))) for s in sums], 1
    )
    sums = jnp.pad(sums, ((0, 0), (0, SPARE - sums.shape[1]), (0, 0)))
    part = width // chips
    if own_copies:
        early = jnp.concatenate([grad_qkv[:, : 3 * head_dim], sums], 1).astype(BF16)
        (early,) = scatter([early], 3)
        grads = [early[n * head_dim : (n + 1) * head_dim] for n in range(3)]
        vector_grads = early[3 * head_dim :]
    else:
        grads = [
            grad_qkv[:, n * head_dim : (n + 1) * head_dim].reshape(chips, part, width)
            for n in range(3)
        ]
        *grads, vector_grads = [
            lax.psum(
                lax.psum_scatter(g.astype(F32), "wide", scatter_dimension=0, tiled=False).astype(
                    BF16
                ),
                "narrow",
            ).astype(F32)
            for g in grads + [sums]
        ]
        late = [
            lax.psum(
                lax.psum_scatter(g.astype(F32), "wide", scatter_dimension=0, tiled=False).astype(
                    BF16
                ),
                "narrow",
            ).astype(F32)
            for g in late
        ]
    g_query, g_key, g_value = [g.T for g in grads]
    g_out, g_hidden, g_proj = [g.T for g in late]
    g_vec = [vector_grads[n, : v.shape[0]] for n, v in enumerate(vectors)]
    return (
        mixed, grad_tokens, g_vec[0], g_vec[1], g_query, g_vec[2], g_key, g_value, g_vec[3],
        g_out, g_vec[4], g_vec[5], g_vec[6], g_hidden, g_vec[7], g_proj, g_vec[8],
    )


def solution(mesh):
    both, wide = P(("wide", "narrow"), None), P("wide")
    weight = P(None, "wide")
    return jax.shard_map(
        functools.partial(shards, mesh.shape["wide"], mesh.shape["narrow"]),
        mesh=mesh,
        in_specs=(
            both, both, both, both, wide, wide, weight, wide, weight, weight, wide, weight, wide,
            wide, wide, weight, wide, weight, wide,
        ),
        out_specs=(
            both, both, wide, wide, weight, wide, weight, weight, wide, weight, wide, wide, wide,
            weight, wide, weight, wide,
        ),
        check_vma=False,
    )
```

```python
import functools
import math

import jax
import jax.numpy as jnp
from jax import lax
from jax.experimental import pallas as pl
from jax.experimental.pallas import tpu as pltpu
from jax.sharding import PartitionSpec as P

HEADS = 16
F32 = jnp.float32
BF16 = jnp.bfloat16
MESH = pl.DeviceIdType.MESH
LOG2E = math.log2(math.e)
MASKED = -1e30
SPARE = 16
SEGS = 4
GATHER_STEPS = (0, 3, 6, 10, 14)
SCATTER_STEPS = (0, 2, 6, 9, 12, 15)
CHUNK = 512


def dims(left, right, a, b):
    return lax.dot_general(left, right, (((a,), (b,)), ((), ())), preferred_element_type=F32)


def chip_axes(chips):
    if chips == 16:
        return ((4, 4), (2, 2), (1, 2))
    return ((1, chips),)


def axis_orders(axes):
    if len(axes) == 3:
        return ((0, 1, 2), (2, 0, 1))
    return (tuple(range(len(axes))),) * 2


def place(me, axis):
    stride, size = axis
    return lax.rem(lax.div(me, stride), size)


def peer(me, axis, step):
    stride, size = axis
    mine = place(me, axis)
    other = lax.rem(mine + step, size)
    return me + (other - mine) * stride


def greet(me, core, axes):
    barrier = pltpu.get_barrier_semaphore()
    count = 1
    pl.semaphore_signal(barrier, 1, device_id=(me, 1 - core), device_id_type=MESH)
    for axis in axes:
        for step in range(1, axis[1]):
            pl.semaphore_signal(
                barrier, 1, device_id=(peer(me, axis, step), core), device_id_type=MESH
            )
            count += 1
    pl.semaphore_wait(barrier, count)


def held_blocks(me, axes, done):
    ids = [me]
    for a in done:
        stride, size = axes[a]
        ids = [i + (v - place(me, axes[a])) * stride for i in ids for v in range(size)]
    return ids


def half(ref, block, c):
    width = ref.shape[-1] // 2
    return ref.at[block, :, pl.ds(c * width, width)]


def flat_half(ref, c):
    width = ref.shape[-1] // 2
    return ref.at[:, pl.ds(c * width, width)]


def gather_plan(ins, outs, sems, me, c, axes):
    order = axis_orders(axes)[c]
    send, recv, pass_send, pass_recv, own = sems
    chips = outs[0].shape[0]
    stages = []
    count = [0]
    passed = [0]
    pending = []

    def hand_over(ids, first=False):
        for n, block in enumerate(ids):
            for k, (src, dst) in enumerate(zip(ins, outs)):
                slot = passed[0] + n * len(outs) + k
                source = flat_half(src, c) if first else half(dst, block, c)
                pltpu.make_async_remote_copy(
                    source, half(dst, block, c), pass_send.at[slot], pass_recv.at[slot],
                    device_id=(me, 1 - c), device_id_type=MESH,
                ).start()
        passed[0] += len(ids) * len(outs)

    def copies(number):
        axis = axes[order[number]]
        ids = held_blocks(me, axes, order[:number])
        base = sum(
            (axes[order[m]][1] - 1) * math.prod(axes[a][1] for a in order[:m]) * len(outs)
            for m in range(number)
        )
        out = []
        slot = base
        for step in range(1, axis[1]):
            target = peer(me, axis, step)
            source = peer(me, axis, axis[1] - step)
            for block in ids:
                for k, (src, dst) in enumerate(zip(ins, outs)):
                    first = number == 0
                    out.append((
                        pltpu.make_async_remote_copy(
                            flat_half(src, c) if first else half(dst, block, c),
                            half(dst, block, c), send.at[slot], recv.at[slot],
                            device_id=(target, c), device_id_type=MESH,
                        ),
                        block + (source - me),
                    ))
                    slot += 1
        return out

    def begin(number):
        for copy, _ in copies(number):
            copy.start()

    def land(number):
        got = copies(number)
        for copy, _ in got:
            copy.wait_recv()
        return [block for _, block in got[:: len(outs)]]

    def first():
        for k, (src, dst) in enumerate(zip(ins, outs)):
            pltpu.make_async_copy(src, dst.at[me], own.at[k]).start()
        begin(0)

    def middle(number):
        def run():
            blocks = land(number)
            if number == 0:
                for k, (src, dst) in enumerate(zip(ins, outs)):
                    pltpu.make_async_copy(src, dst.at[me], own.at[k]).wait()
            if number + 1 < len(order):
                begin(number + 1)
            hand_over(blocks)
        return run

    def last():
        total = (chips - 1) * len(outs)
        for number in range(len(order)):
            for copy, _ in copies(number):
                copy.wait_send()
        for k in range(total):
            dst = outs[k % len(outs)]
            pltpu.make_async_remote_copy(
                half(dst, me, c), half(dst, me, 1 - c), pass_send.at[k], pass_recv.at[k],
                device_id=(me, 1 - c), device_id_type=MESH,
            ).wait()

    stages.append(first)
    for number in range(len(order)):
        stages.append(middle(number))
    stages.append(last)
    return stages


def gather_sems(chips, arrays):
    total = (chips - 1) * arrays
    return [pltpu.SemaphoreType.DMA((total,)) for _ in range(4)] + [
        pltpu.SemaphoreType.DMA((arrays,))
    ]


def gather_kernel(chips, arrays, *refs):
    ins, outs, sems = refs[:arrays], refs[arrays : 2 * arrays], refs[2 * arrays :]
    me, core = lax.axis_index("wide"), lax.axis_index("narrow")
    axes = chip_axes(chips)
    greet(me, core, axes)
    for c in range(2):
        @pl.when(core == c)
        def _():
            for stage in gather_plan(ins, outs, sems, me, c, axes):
                stage()


def gather(arrays, chips, ident):
    vm = pl.BlockSpec(memory_space=pltpu.VMEM)
    return pl.pallas_call(
        functools.partial(gather_kernel, chips, len(arrays)),
        out_shape=[jax.ShapeDtypeStruct((chips,) + a.shape, a.dtype) for a in arrays],
        in_specs=[vm] * len(arrays),
        out_specs=[pl.BlockSpec(memory_space=pl.ANY)] * len(arrays),
        scratch_shapes=gather_sems(chips, len(arrays)),
        compiler_params=pltpu.CompilerParams(collective_id=ident, has_side_effects=True),
    )(*arrays)


def phase_base(axes, order, number, arrays):
    return sum(
        (axes[order[m]][1] - 1) * math.prod(axes[a][1] for a in order[:m]) * arrays
        for m in range(number)
    )


def scatter_plan(ins, outs, accs, halves, landed, results, sems, me, c, axes):
    order = axis_orders(axes)[c]
    send, recv, swap_send, swap_recv, own, out_sem = sems
    arrays = len(ins)

    def swap():
        copies = []
        for k in range(arrays):
            width = ins[k].shape[-1] // 2
            copies.append((
                pltpu.make_async_remote_copy(
                    ins[k].at[:, :, pl.ds((1 - c) * width, width)], halves[k],
                    swap_send.at[k], swap_recv.at[k],
                    device_id=(me, 1 - c), device_id_type=MESH,
                ),
                pltpu.make_async_copy(
                    ins[k].at[:, :, pl.ds(c * width, width)], accs[k], own.at[k]
                ),
            ))
        return copies

    def copies(number):
        axis = axes[order[number]]
        ids = held_blocks(me, axes, order[:number])
        slot = phase_base(axes, order, number, 1)
        out = []
        for step in range(1, axis[1]):
            target = peer(me, axis, step)
            for block in ids:
                for k in range(arrays):
                    n = slot * arrays + k
                    out.append((
                        pltpu.make_async_remote_copy(
                            accs[k].at[block + (target - me)], landed[k].at[slot],
                            send.at[n], recv.at[n],
                            device_id=(target, c), device_id_type=MESH,
                        ),
                        block, k, slot,
                    ))
                slot += 1
        return out

    def begin(number):
        for copy, *_ in copies(number):
            copy.start()

    def first():
        for remote, local in swap():
            remote.start()
            local.start()

    def add_pair():
        for remote, local in swap():
            local.wait()
            remote.wait()
        for k in range(arrays):
            @pl.loop(0, accs[k].shape[0])
            def _(block):
                accs[k][block] = (
                    accs[k][block].astype(F32) + halves[k][block].astype(F32)
                ).astype(BF16)
        begin(len(order) - 1)

    def add(number):
        def run():
            got = copies(number)
            for copy, *_ in got:
                copy.wait()
            groups = {}
            for position, (_, block, k, slot) in enumerate(got):
                ids = math.prod(axes[a][1] for a in order[:number])
                groups.setdefault((position // arrays % ids, k), (block, []))[1].append(slot)
            for (_, k), (block, slots) in groups.items():
                total = accs[k][block].astype(F32)
                for slot in slots:
                    total = total + landed[k][slot].astype(F32)
                if number:
                    accs[k][block] = total.astype(BF16)
                else:
                    width = total.shape[-1]
                    results[k][:, pl.ds(c * width, width)] = total
            if number:
                begin(number - 1)
            else:
                for copy in finals():
                    copy.start()
        return run

    def finals():
        return [
            pltpu.make_async_remote_copy(
                flat_half(results[k], c), flat_half(results[k], c),
                swap_send.at[arrays + k], swap_recv.at[arrays + k],
                device_id=(me, 1 - c), device_id_type=MESH,
            )
            for k in range(arrays)
        ]

    def last():
        outgoing = [pltpu.make_async_copy(results[k], outs[k], out_sem.at[k]) for k in range(arrays)]
        for copy, out in zip(finals(), outgoing):
            copy.wait()
            out.start()
        for out in outgoing:
            out.wait()

    return [first, add_pair] + [add(n) for n in reversed(range(len(order)))] + [last]


def scatter_scratch(arrays):
    chips = arrays[0].shape[0]
    number = len(arrays)
    scratch = []
    for rows in (chips, chips, chips - 1):
        scratch += [pltpu.VMEM((rows, a.shape[1], a.shape[2] // 2), BF16) for a in arrays]
    scratch += [pltpu.VMEM(a.shape[1:], F32) for a in arrays]
    dma = pltpu.SemaphoreType.DMA
    return scratch + [dma(((chips - 1) * number,)) for _ in range(2)] + [
        dma((n,)) for n in (2 * number, 2 * number, number, number)
    ]


def scatter_parts(arrays, refs):
    parts = [refs[n * arrays : (n + 1) * arrays] for n in range(4)]
    return parts, refs[4 * arrays :]


def scatter_kernel(chips, arrays, *refs):
    ins, outs = refs[:arrays], refs[arrays : 2 * arrays]
    parts, sems = scatter_parts(arrays, refs[2 * arrays :])
    me, core = lax.axis_index("wide"), lax.axis_index("narrow")
    axes = chip_axes(chips)
    greet(me, core, axes)
    for c in range(2):
        @pl.when(core == c)
        def _():
            for stage in scatter_plan(ins, outs, *parts, sems, me, c, axes):
                stage()


def scatter(arrays, ident):
    any_space = pl.BlockSpec(memory_space=pl.ANY)
    return pl.pallas_call(
        functools.partial(scatter_kernel, arrays[0].shape[0], len(arrays)),
        out_shape=[jax.ShapeDtypeStruct(a.shape[1:], F32) for a in arrays],
        in_specs=[any_space] * len(arrays),
        out_specs=[any_space] * len(arrays),
        scratch_shapes=scatter_scratch(arrays),
        compiler_params=pltpu.CompilerParams(
            collective_id=ident, has_side_effects=True, vmem_limit_bytes=60 * 2**20
        ),
    )(*arrays)


def forward_head(qkv, extra, pad, out, lse, head_dim):
    count = qkv.shape[-1]
    factor = head_dim**-0.5 * LOG2E
    keys = jnp.concatenate([qkv[0, head_dim : 2 * head_dim, :], extra[1]], 0).T
    value = qkv[0, 2 * head_dim : 3 * head_dim + SPARE, :]

    for start in range(0, count, CHUNK):
        part = pl.ds(start, CHUNK)
        query = qkv[0, :head_dim, part]
        own_key = qkv[0, head_dim : 2 * head_dim, part]
        own = jnp.sum(query.astype(F32) * own_key.astype(F32), 0, keepdims=True) + pad[:, part]
        raw = dims(keys, jnp.concatenate([query, extra[0, :, part]], 0), 1, 0)
        top = jnp.maximum(jnp.max(raw, 0, keepdims=True), own)
        probs = jnp.exp2((raw - top) * factor).astype(BF16)
        own = jnp.exp2((own - top) * factor)
        both = dims(value, probs, 1, 0)
        total = both[head_dim : head_dim + 1] + own
        own_value = qkv[0, 2 * head_dim : 3 * head_dim, part].astype(F32)
        out[0, :, part] = ((both[:head_dim] + own * own_value) / total).astype(BF16)
        lse[0, :, part] = top + jnp.log2(total) * (1.0 / factor)


def split_rows(row):
    high = row.astype(BF16)
    rest = row - high.astype(F32)
    middle = rest.astype(BF16)
    low = (rest - middle.astype(F32)).astype(BF16)
    return [high, middle, low]


def backward_head(qkv, extra, pad, out, d_out, lse, grad, d_key, d_value, head_dim):
    count = qkv.shape[-1]
    scale = head_dim**-0.5
    factor = scale * LOG2E
    keys = qkv[0, head_dim : 2 * head_dim, :]
    keys_t = jnp.concatenate([keys, extra[1]], 0).T
    row = lax.broadcasted_iota(jnp.int32, (SPARE, count), 0)
    ones = jnp.where(row < 3, 1.0, 0.0).astype(BF16)
    value_t = jnp.concatenate([qkv[0, 2 * head_dim : 3 * head_dim, :], ones], 0).T

    for start in range(0, count, CHUNK):
        part = pl.ds(start, CHUNK)
        query = qkv[0, :head_dim, part]
        d_part = d_out[0, :, part]
        d_full = d_part.astype(F32)
        share = jnp.sum(d_full * out[0, :, part].astype(F32), 0, keepdims=True)
        row = lax.broadcasted_iota(jnp.int32, (SPARE, CHUNK), 0)

        def spread(values, at, base):
            for n, piece in enumerate(split_rows(values)):
                base = jnp.where(row == at + n, -piece.astype(F32), base)
            return base.astype(BF16)

        base = extra[0, :, part].astype(F32)
        query_x = jnp.concatenate([query, spread(lse[0, :, part], 5, base)], 0)
        d_part_x = jnp.concatenate([d_part, spread(share, 0, jnp.zeros_like(base))], 0)
        probs = jnp.exp2(dims(keys_t, query_x, 1, 0) * factor)
        d_scores = (probs * dims(value_t, d_part_x, 1, 0)).astype(BF16)
        probs_low = probs.astype(BF16)

        own_key = qkv[0, head_dim : 2 * head_dim, part].astype(F32)
        own_value = qkv[0, 2 * head_dim : 3 * head_dim, part].astype(F32)
        query_f = query.astype(F32)
        own = jnp.sum(query_f * own_key, 0, keepdims=True) + pad[:, part]
        own = jnp.exp2((own - lse[0, :, part]) * factor)
        own_ds = own * (jnp.sum(d_full * own_value, 0, keepdims=True) - share)

        grad[0, :head_dim, part] = (
            (dims(keys, d_scores, 1, 0) + own_ds * own_key) * scale
        ).astype(BF16)
        more_value = dims(d_part, probs_low, 1, 1)
        more_key = dims(query, d_scores, 1, 1)
        if start == 0:
            d_value[...] = more_value
            d_key[...] = more_key
        else:
            d_value[...] += more_value
            d_key[...] += more_key
        grad[0, head_dim : 2 * head_dim, part] = (own_ds * query_f).astype(BF16)
        grad[0, 2 * head_dim : 3 * head_dim, part] = (own * d_full).astype(BF16)
    for slot, total, factor_out in ((1, d_key, scale), (2, d_value, 1.0)):
        rows = pl.ds(slot * head_dim, head_dim)
        whole = total[...]
        grad[0, rows, :] = ((whole + grad[0, rows, :].astype(F32)) * factor_out).astype(BF16)
    grad[0, 3 * head_dim :, :] = jnp.zeros((SPARE, count), BF16)


def head_spec(rows, count):
    return pl.BlockSpec((1, rows, count), lambda h: (h, 0, 0))


def same(*shape):
    return pl.BlockSpec(shape, lambda h: (0,) * len(shape))


def run_stages(plan, when, chips):
    me, core = lax.axis_index("wide"), lax.axis_index("narrow")
    axes = chip_axes(chips)
    h = pl.program_id(0)

    @pl.when(h == 0)
    def _():
        greet(me, core, axes)

    for c in range(2):
        for stage, step in zip(plan(me, c, axes), when):
            @pl.when((core == c) & (h == step))
            def _(stage=stage):
                stage()


def attention(qkv, extra, pad, weights=(), chips=0, ident=None):
    rows, count = qkv.shape[1:]
    head_dim = (rows - SPARE) // 3
    n = len(weights)

    def body(*refs):
        (qkv_ref, extra_ref, pad_ref), ins = refs[:3], refs[3 : 3 + n]
        (out, lse), outs, sems = refs[3 + n : 5 + n], refs[5 + n : 5 + 2 * n], refs[5 + 2 * n :]
        if n:
            run_stages(
                lambda me, c, axes: gather_plan(ins, outs, sems, me, c, axes),
                GATHER_STEPS, chips,
            )
        forward_head(qkv_ref, extra_ref, pad_ref, out, lse, head_dim)

    return pl.pallas_call(
        body,
        grid=(HEADS,),
        out_shape=[
            jax.ShapeDtypeStruct((HEADS, head_dim, count), BF16),
            jax.ShapeDtypeStruct((HEADS, 1, count), F32),
        ]
        + [jax.ShapeDtypeStruct((chips,) + a.shape, a.dtype) for a in weights],
        in_specs=[head_spec(rows, count), same(2, SPARE, count), same(1, count)]
        + [same(*a.shape) for a in weights],
        out_specs=[head_spec(head_dim, count), head_spec(1, count)]
        + [pl.BlockSpec(memory_space=pl.ANY)] * n,
        scratch_shapes=gather_sems(chips, n) if n else [],
        compiler_params=pltpu.CompilerParams(
            vmem_limit_bytes=60 * 2**20, collective_id=ident, has_side_effects=n > 0
        ),
    )(qkv, extra, pad, *weights)


def attention_back(qkv, extra, pad, out, d_out, lse, grads=(), chips=0, ident=None):
    rows, count = qkv.shape[1:]
    head_dim = (rows - SPARE) // 3
    n = len(grads)

    def body(*refs):
        ins, refs = refs[:6], refs[6:]
        g_ins, grad, g_outs, rest = refs[:n], refs[n], refs[n + 1 : 2 * n + 1], refs[2 * n + 1 :]
        d_key, d_value = rest[:2]
        if n:
            parts, sems = scatter_parts(n, rest[2:])
            run_stages(
                lambda me, c, axes: scatter_plan(g_ins, g_outs, *parts, sems, me, c, axes),
                SCATTER_STEPS, chips,
            )
        backward_head(*ins, grad, d_key, d_value, head_dim)

    any_space = pl.BlockSpec(memory_space=pl.ANY)
    return pl.pallas_call(
        body,
        grid=(HEADS,),
        out_shape=[jax.ShapeDtypeStruct((HEADS, rows, count), BF16)]
        + [jax.ShapeDtypeStruct(a.shape[1:], F32) for a in grads],
        in_specs=[
            head_spec(rows, count),
            same(2, SPARE, count),
            same(1, count),
            head_spec(head_dim, count),
            head_spec(head_dim, count),
            head_spec(1, count),
        ]
        + [any_space] * n,
        out_specs=[head_spec(rows, count)] + [any_space] * n,
        scratch_shapes=[pltpu.VMEM((head_dim, count), F32)] * 2
        + (scatter_scratch(grads) if n else []),
        compiler_params=pltpu.CompilerParams(
            vmem_limit_bytes=60 * 2**20, collective_id=ident, has_side_effects=n > 0
        ),
    )(qkv, extra, pad, out, d_out, lse, *grads)


def masking_rows(seg, live):
    n = jnp.arange(SPARE)[:, None]
    seg, live = seg[None], live[None]
    group = n < SEGS
    query = jnp.where(group, seg == n, n == SEGS).astype(F32)
    keys = jnp.where(
        group,
        jnp.where(seg == n, 0.0, MASKED),
        jnp.where(
            n == SEGS,
            jnp.where(live > 0, 0.0, MASKED),
            jnp.where((n > SEGS) & (n < SEGS + 4), 1.0, 0.0),
        ),
    )
    return jnp.stack([query, keys]).astype(BF16), jnp.where(live > 0, MASKED, 0.0).astype(F32)


def norm(values):
    centred = values - jnp.mean(values, -1, keepdims=True)
    factor = lax.rsqrt(jnp.mean(centred * centred, -1, keepdims=True) + 1e-05)
    return centred * factor, factor


def norm_back(grad, normed, factor, gain):
    scaled = grad * gain
    inner = (
        scaled
        - jnp.mean(scaled, -1, keepdims=True)
        - normed * jnp.mean(scaled * normed, -1, keepdims=True)
    )
    return factor * inner, jnp.sum(grad * normed, 0), jnp.sum(grad, 0)


def gelu_pair(values):
    cdf = 0.5 * (1.0 + lax.erf(values * (1.0 / math.sqrt(2.0))))
    pdf = jnp.exp(-0.5 * values * values) * (1.0 / math.sqrt(2.0 * math.pi))
    return values * cdf, cdf + values * pdf


def row_sums(values):
    return jnp.sum(values.astype(F32), 0)


def widen(vector, width):
    return jnp.pad(vector, (0, width - vector.shape[0]))


def shards(
    chips,
    replicas,
    tokens,
    segment,
    keep,
    cotangent,
    gain_one,
    bias_one,
    w_query,
    b_query,
    w_key,
    w_value,
    b_value,
    w_out,
    b_out,
    gain_two,
    bias_two,
    w_hidden,
    b_hidden,
    w_proj,
    b_proj,
):
    own_copies = chips == HEADS and replicas == 2
    count, width = tokens.shape
    head_dim = width // HEADS
    hidden = w_hidden.shape[1] * chips
    vectors = (gain_one, bias_one, b_query, b_value, b_out, gain_two, bias_two, b_hidden, b_proj)
    packed = jnp.stack([widen(v, width) for v in vectors])
    packed = jnp.pad(packed, ((0, SPARE - len(vectors)), (0, 0)))

    if own_copies:
        first = jnp.concatenate([w_query.T, w_key.T, w_value.T, packed], 0)
        (first,) = gather([first], chips, 0)
        joined_t = first
        vector_rows = first[:, 3 * head_dim :, :]
    else:
        whole = [
            lax.all_gather(w.T, "wide", axis=0, tiled=True) for w in (w_query, w_key, w_value)
        ]
        whole = [w.reshape(HEADS, head_dim, width) for w in whole]
        whole.append(jnp.zeros((HEADS, SPARE, width), BF16))
        joined_t = jnp.concatenate(whole, 1)
        vector_rows = lax.all_gather(packed, "wide", axis=0, tiled=False)
        out_t, hidden_t, proj_t = [
            lax.all_gather(w.T, "wide", axis=0, tiled=False) for w in (w_out, w_hidden, w_proj)
        ]
    joined_t = joined_t.reshape(HEADS * (3 * head_dim + SPARE), width)
    gain_one_f, bias_one_f, b_query_f, b_value_f, b_out_f, gain_two_f, bias_two_f, b_hidden_f, b_proj_f = [
        vector_rows[:, n, : v.shape[0]].reshape(-1).astype(F32) for n, v in enumerate(vectors)
    ]

    live = keep[0]
    seg = segment[0]
    extra, pad = masking_rows(seg, live)

    x = tokens.astype(F32)
    xhat_one, factor_one = norm(x)
    h_one = (xhat_one * gain_one_f + bias_one_f).astype(BF16)
    block = 3 * head_dim + SPARE
    offsets = jnp.concatenate(
        [
            b_query_f.reshape(HEADS, head_dim),
            jnp.zeros((HEADS, head_dim), F32),
            b_value_f.reshape(HEADS, head_dim),
            jnp.zeros((HEADS, SPARE), F32),
        ],
        1,
    )
    row = jnp.arange(block)[None, :, None]
    qkv = dims(joined_t, h_one, 1, 1).reshape(HEADS, block, count) + offsets[:, :, None]
    qkv = jnp.where(row < 3 * head_dim, qkv, jnp.where(row == 3 * head_dim, 1.0, 0.0)).astype(BF16)
    if own_copies:
        o_t, lse, out_t, hidden_t, proj_t = attention(
            qkv, extra, pad, (w_out.T, w_hidden.T, w_proj.T), chips, 1
        )
    else:
        o_t, lse = attention(qkv, extra, pad)
    out_t = out_t.reshape(width, width)
    hidden_t = hidden_t.reshape(hidden, width)
    proj_t = proj_t.reshape(width, hidden)
    o_flat = o_t.reshape(width, count)
    x_one = x + dims(o_flat, out_t, 0, 1) + b_out_f
    xhat_two, factor_two = norm(x_one)
    h_two = (xhat_two * gain_two_f + bias_two_f).astype(BF16)
    upper = dims(h_two, hidden_t, 1, 1) + b_hidden_f
    act, slope = [v.astype(BF16) for v in gelu_pair(upper)]
    mixed = (x_one + dims(act, proj_t, 1, 1) + b_proj_f).astype(BF16)

    d_y = cotangent.astype(F32) * live.astype(F32)[:, None]
    d_m = d_y.astype(BF16)
    grad_proj = dims(d_m, act, 0, 0).astype(BF16)
    d_upper = (dims(d_m, proj_t, 1, 0) * slope.astype(F32)).astype(BF16)
    grad_hidden = dims(d_upper, h_two, 0, 0).astype(BF16)
    d_two, grad_gain_two, grad_bias_two = norm_back(
        dims(d_upper, hidden_t, 1, 0), xhat_two, factor_two, gain_two_f
    )
    d_x_one = d_y + d_two
    d_attn = d_x_one.astype(BF16)
    grad_out = dims(d_attn, o_flat, 0, 1).astype(BF16)
    d_o = dims(out_t, d_attn, 0, 1).astype(BF16).reshape(HEADS, head_dim, count)
    late = [
        g.reshape(chips, -1, g.shape[-1]) for g in (grad_out, grad_hidden, grad_proj)
    ]
    if own_copies:
        d_qkv, *late = attention_back(qkv, extra, pad, o_t, d_o, lse, late, chips, 2)
    else:
        (d_qkv,) = attention_back(qkv, extra, pad, o_t, d_o, lse)
    d_flat = d_qkv.reshape(HEADS * block, count)
    grad_qkv = dims(d_flat, h_one, 1, 0).reshape(HEADS, block, width)
    bias_sums = jnp.sum(d_qkv.astype(F32), -1)
    d_one, grad_gain_one, grad_bias_one = norm_back(
        dims(d_flat, joined_t, 0, 0), xhat_one, factor_one, gain_one_f
    )
    grad_tokens = d_x_one + d_one

    sums = (
        grad_gain_one,
        grad_bias_one,
        bias_sums[:, :head_dim].reshape(-1),
        bias_sums[:, 2 * head_dim : 3 * head_dim].reshape(-1),
        row_sums(d_attn),
        grad_gain_two,
        grad_bias_two,
        row_sums(d_upper),
        row_sums(d_m),
    )
    sums = jnp.stack(
        [jnp.pad(s.reshape(chips, -1), ((0, 0), (0, width - s.size // chips))) for s in sums], 1
    )
    sums = jnp.pad(sums, ((0, 0), (0, SPARE - sums.shape[1]), (0, 0)))
    part = width // chips
    if own_copies:
        early = jnp.concatenate([grad_qkv[:, : 3 * head_dim], sums], 1).astype(BF16)
        (early,) = scatter([early], 3)
        grads = [early[n * head_dim : (n + 1) * head_dim] for n in range(3)]
        vector_grads = early[3 * head_dim :]
    else:
        grads = [
            grad_qkv[:, n * head_dim : (n + 1) * head_dim].reshape(chips, part, width)
            for n in range(3)
        ]
        *grads, vector_grads = [
            lax.psum(
                lax.psum_scatter(g.astype(F32), "wide", scatter_dimension=0, tiled=False).astype(
                    BF16
                ),
                "narrow",
            ).astype(F32)
            for g in grads + [sums]
        ]
        late = [
            lax.psum(
                lax.psum_scatter(g.astype(F32), "wide", scatter_dimension=0, tiled=False).astype(
                    BF16
                ),
                "narrow",
            ).astype(F32)
            for g in late
        ]
    g_query, g_key, g_value = [g.T for g in grads]
    g_out, g_hidden, g_proj = [g.T for g in late]
    g_vec = [vector_grads[n, : v.shape[0]] for n, v in enumerate(vectors)]
    return (
        mixed, grad_tokens, g_vec[0], g_vec[1], g_query, g_vec[2], g_key, g_value, g_vec[3],
        g_out, g_vec[4], g_vec[5], g_vec[6], g_hidden, g_vec[7], g_proj, g_vec[8],
    )


def solution(mesh):
    both, wide = P(("wide", "narrow"), None), P("wide")
    weight = P(None, "wide")
    return jax.shard_map(
        functools.partial(shards, mesh.shape["wide"], mesh.shape["narrow"]),
        mesh=mesh,
        in_specs=(
            both, both, both, both, wide, wide, weight, wide, weight, weight, wide, weight, wide,
            wide, wide, weight, wide, weight, wide,
        ),
        out_specs=(
            both, both, wide, wide, weight, wide, weight, weight, wide, weight, wide, wide, wide,
            weight, wide, weight, wide,
        ),
        check_vma=False,
    )
```

```python
import functools
import itertools
import math

import jax
import jax.numpy as jnp
from jax import lax
from jax.experimental import pallas as pl
from jax.experimental.pallas import tpu as pltpu
from jax.sharding import PartitionSpec as P

HEADS = 16
F32 = jnp.float32
BF16 = jnp.bfloat16
MESH = pl.DeviceIdType.MESH
LOG2E = math.log2(math.e)
MASKED = -1e30
SPARE = 16
SEGS = 4
GATHER_STEPS = (1, HEADS)
SCATTER_STEPS = (0, HEADS)
CHUNK = 512


def dims(left, right, a, b):
    return lax.dot_general(left, right, (((a,), (b,)), ((), ())), preferred_element_type=F32)


def chip_axes(chips):
    if chips == 16:
        return ((4, 4), (2, 2), (1, 2))
    return ((1, chips),)


def axis_orders(axes):
    if len(axes) == 3:
        return ((0, 1, 2), (2, 0, 1))
    return (tuple(range(len(axes))),) * 2


def place(me, axis):
    stride, size = axis
    return lax.rem(lax.div(me, stride), size)


def peer(me, axis, step):
    stride, size = axis
    mine = place(me, axis)
    other = lax.rem(mine + step, size)
    return me + (other - mine) * stride


def greet(me, core, axes):
    barrier = pltpu.get_barrier_semaphore()
    count = 1
    pl.semaphore_signal(barrier, 1, device_id=(me, 1 - core), device_id_type=MESH)
    for axis in axes:
        for step in range(1, axis[1]):
            pl.semaphore_signal(
                barrier, 1, device_id=(peer(me, axis, step), core), device_id_type=MESH
            )
            count += 1
    pl.semaphore_wait(barrier, count)


def moved(me, axes, order, steps, sign):
    for a, step in zip(order, steps):
        size = axes[a][1]
        if step:
            other = peer(me, axes[a], step if sign > 0 else size - step)
            me = me + (other - me)
    return me


def grid_of(axes, order):
    return [range(axes[a][1]) for a in order]


def slots_of(axes, order):
    slots = {}
    for k in range(len(order)):
        for steps in itertools.product(*grid_of(axes, order[: k + 1])):
            if steps[-1]:
                slots[steps] = len(slots)
    return slots


def half(ref, block, c):
    width = ref.shape[-1] // 2
    return ref.at[block, :, pl.ds(c * width, width)]


def flat_half(ref, c):
    width = ref.shape[-1] // 2
    return ref.at[:, pl.ds(c * width, width)]


def gather_plan(ins, outs, sems, me, c, axes):
    order = axis_orders(axes)[c]
    send, recv, pass_send, pass_recv, own = sems
    arrays = len(outs)
    slots = slots_of(axes, order)

    def block_of(steps):
        return moved(me, axes, order, steps, -1)

    def message(steps):
        before = steps[:-1]
        target = moved(me, axes, order[len(before) :], steps[-1:], 1)
        block = block_of(before)
        fresh = not any(before)
        return [
            pltpu.make_async_remote_copy(
                flat_half(src, c) if fresh else half(dst, block, c),
                half(dst, block, c),
                send.at[slots[steps] * arrays + k],
                recv.at[slots[steps] * arrays + k],
                device_id=(target, c), device_id_type=MESH,
            )
            for k, (src, dst) in enumerate(zip(ins, outs))
        ]

    def send_on(steps):
        for k in range(len(steps), len(order)):
            lead = steps + (0,) * (k - len(steps))
            for step in range(1, axes[order[k]][1]):
                for copy in message(lead + (step,)):
                    copy.start()

    def hand_over(steps):
        block = block_of(steps)
        return [
            pltpu.make_async_remote_copy(
                half(dst, block, c), half(dst, block, c),
                pass_send.at[slots[steps] * arrays + k], pass_recv.at[slots[steps] * arrays + k],
                device_id=(me, 1 - c), device_id_type=MESH,
            )
            for k, dst in enumerate(outs)
        ]

    def keep_own():
        return [pltpu.make_async_copy(s, d.at[me], own.at[k]) for k, (s, d) in enumerate(zip(ins, outs))]

    def first():
        send_on(())
        for copy in keep_own():
            copy.start()

    def arrive(steps):
        def run():
            for copy in message(steps):
                copy.wait_recv()
            send_on(steps)
            for copy in hand_over(steps):
                copy.start()
        return run

    def last():
        for copy in keep_own():
            copy.wait()
        for steps in slots:
            for copy in message(steps):
                copy.wait_send()
            for copy in hand_over(steps):
                copy.wait_send()
        other = axis_orders(axes)[1 - c]
        other_slots = slots_of(axes, other)
        for steps, slot in other_slots.items():
            block = moved(me, axes, other, steps, -1)
            for k, dst in enumerate(outs):
                n = slot * arrays + k
                pltpu.make_async_remote_copy(
                    half(dst, block, 1 - c), half(dst, block, 1 - c),
                    pass_send.at[n], pass_recv.at[n],
                    device_id=(me, 1 - c), device_id_type=MESH,
                ).wait_recv()

    def cost(steps):
        return (sum(1 for s in steps if s), len(steps), steps)

    return [first] + [arrive(steps) for steps in sorted(slots, key=cost)] + [last]


def gather_sems(chips, arrays):
    total = (chips - 1) * arrays
    return [pltpu.SemaphoreType.DMA((total,)) for _ in range(4)] + [
        pltpu.SemaphoreType.DMA((arrays,))
    ]


def gather_kernel(chips, arrays, *refs):
    ins, outs, sems = refs[:arrays], refs[arrays : 2 * arrays], refs[2 * arrays :]
    me, core = lax.axis_index("wide"), lax.axis_index("narrow")
    axes = chip_axes(chips)
    greet(me, core, axes)
    for c in range(2):
        @pl.when(core == c)
        def _():
            for stage in gather_plan(ins, outs, sems, me, c, axes):
                stage()


def gather(arrays, chips, ident):
    vm = pl.BlockSpec(memory_space=pltpu.VMEM)
    return pl.pallas_call(
        functools.partial(gather_kernel, chips, len(arrays)),
        out_shape=[jax.ShapeDtypeStruct((chips,) + a.shape, a.dtype) for a in arrays],
        in_specs=[vm] * len(arrays),
        out_specs=[pl.BlockSpec(memory_space=pl.ANY)] * len(arrays),
        scratch_shapes=gather_sems(chips, len(arrays)),
        compiler_params=pltpu.CompilerParams(collective_id=ident, has_side_effects=True),
    )(*arrays)


def scatter_plan(ins, outs, accs, halves, landed, results, sems, me, c, axes):
    order = axis_orders(axes)[c]
    send, recv, swap_send, swap_recv, own, out_sem, last_send, last_recv = sems
    arrays = len(ins)
    slots = slots_of(axes, order)
    depth = len(order)

    def all_steps(number):
        steps = itertools.product(*grid_of(axes, order[:number]))
        return sorted(steps, key=lambda t: (-sum(1 for s in t if s), [-s for s in reversed(t)]))

    def owner(steps):
        return moved(me, axes, order, steps, 1)

    whole = all_steps(depth)

    def swap(steps, core):
        there = axis_orders(axes)[core]
        names = all_steps_of(there)
        n = names.index(steps)
        block = moved(me, axes, there, steps, 1)
        return [
            pltpu.make_async_remote_copy(
                half(ins[k], block, core), halves[k].at[block],
                swap_send.at[n * arrays + k], swap_recv.at[n * arrays + k],
                device_id=(me, 1 - c), device_id_type=MESH,
            )
            for k in range(arrays)
        ]

    def all_steps_of(there):
        steps = itertools.product(*grid_of(axes, there))
        return sorted(steps, key=lambda t: (-sum(1 for s in t if s), [-s for s in reversed(t)]))

    def load(steps):
        block = owner(steps)
        n = whole.index(steps)
        return [
            pltpu.make_async_copy(half(ins[k], block, c), accs[k].at[block], own.at[n * arrays + k])
            for k in range(arrays)
        ]

    def message(steps):
        block = owner(steps)
        target = moved(me, axes, order[len(steps) - 1 :], steps[-1:], 1)
        slot = slots[steps]
        return [
            pltpu.make_async_remote_copy(
                accs[k].at[block], landed[k].at[slot],
                send.at[slot * arrays + k], recv.at[slot * arrays + k],
                device_id=(target, c), device_id_type=MESH,
            )
            for k in range(arrays)
        ]

    def send_on(steps):
        if steps and steps[-1]:
            for copy in message(steps):
                copy.start()

    def first():
        for steps in all_steps_of(axis_orders(axes)[1 - c]):
            for copy in swap(steps, 1 - c):
                copy.start()
        for steps in whole:
            for copy in load(steps):
                copy.start()

    def add_pair(steps):
        def run():
            for copy in load(steps):
                copy.wait()
            for copy in swap(steps, c):
                copy.wait_recv()
            block = owner(steps)
            for k in range(arrays):
                accs[k][block] = (
                    accs[k][block].astype(F32) + halves[k][block].astype(F32)
                ).astype(BF16)
            send_on(steps)
        return run

    def add(steps):
        def run():
            got = [steps + (s,) for s in range(1, axes[order[len(steps)]][1])]
            for came in got:
                for copy in message(came):
                    copy.wait_recv()
            block = owner(steps)
            for k in range(arrays):
                total = accs[k][block].astype(F32)
                for came in got:
                    total = total + landed[k][slots[came]].astype(F32)
                if steps:
                    accs[k][block] = total.astype(BF16)
                else:
                    width = total.shape[-1]
                    results[k][:, pl.ds(c * width, width)] = total
            if steps:
                send_on(steps)
            else:
                for copy in finals(c):
                    copy.start()
        return run

    def finals(core):
        return [
            pltpu.make_async_remote_copy(
                flat_half(results[k], core), flat_half(results[k], core),
                last_send.at[k], last_recv.at[k],
                device_id=(me, 1 - c), device_id_type=MESH,
            )
            for k in range(arrays)
        ]

    def last():
        for steps in slots:
            for copy in message(steps):
                copy.wait_send()
        for steps in all_steps_of(axis_orders(axes)[1 - c]):
            for copy in swap(steps, 1 - c):
                copy.wait_send()
        outgoing = [pltpu.make_async_copy(results[k], outs[k], out_sem.at[k]) for k in range(arrays)]
        for copy in finals(c):
            copy.wait_send()
        for copy, out in zip(finals(1 - c), outgoing):
            copy.wait_recv()
            out.start()
        for out in outgoing:
            out.wait()

    events = [first] + [add_pair(steps) for steps in whole]
    for number in reversed(range(depth)):
        events += [add(steps) for steps in all_steps(number)]
    return events + [last]


def scatter_scratch(arrays):
    chips = arrays[0].shape[0]
    number = len(arrays)
    scratch = []
    for rows in (chips, chips, chips - 1):
        scratch += [pltpu.VMEM((rows, a.shape[1], a.shape[2] // 2), BF16) for a in arrays]
    scratch += [pltpu.VMEM(a.shape[1:], F32) for a in arrays]
    dma = pltpu.SemaphoreType.DMA
    sizes = (chips - 1,) * 2 + (chips,) * 3 + (1,) * 3
    return scratch + [dma((n * number,)) for n in sizes]


def scatter_parts(arrays, refs):
    parts = [refs[n * arrays : (n + 1) * arrays] for n in range(4)]
    return parts, refs[4 * arrays :]


def scatter_kernel(chips, arrays, *refs):
    ins, outs = refs[:arrays], refs[arrays : 2 * arrays]
    parts, sems = scatter_parts(arrays, refs[2 * arrays :])
    me, core = lax.axis_index("wide"), lax.axis_index("narrow")
    axes = chip_axes(chips)
    greet(me, core, axes)
    for c in range(2):
        @pl.when(core == c)
        def _():
            for stage in scatter_plan(ins, outs, *parts, sems, me, c, axes):
                stage()


def scatter(arrays, ident):
    any_space = pl.BlockSpec(memory_space=pl.ANY)
    return pl.pallas_call(
        functools.partial(scatter_kernel, arrays[0].shape[0], len(arrays)),
        out_shape=[jax.ShapeDtypeStruct(a.shape[1:], F32) for a in arrays],
        in_specs=[any_space] * len(arrays),
        out_specs=[any_space] * len(arrays),
        scratch_shapes=scatter_scratch(arrays),
        compiler_params=pltpu.CompilerParams(
            collective_id=ident, has_side_effects=True, vmem_limit_bytes=60 * 2**20
        ),
    )(*arrays)


def forward_head(qkv, extra, pad, out, lse, head_dim):
    count = qkv.shape[-1]
    factor = head_dim**-0.5 * LOG2E
    keys = jnp.concatenate([qkv[0, head_dim : 2 * head_dim, :], extra[1]], 0).T
    value = qkv[0, 2 * head_dim : 3 * head_dim + SPARE, :]

    for start in range(0, count, CHUNK):
        part = pl.ds(start, CHUNK)
        query = qkv[0, :head_dim, part]
        own_key = qkv[0, head_dim : 2 * head_dim, part]
        own = jnp.sum(query.astype(F32) * own_key.astype(F32), 0, keepdims=True) + pad[:, part]
        raw = dims(keys, jnp.concatenate([query, extra[0, :, part]], 0), 1, 0)
        top = jnp.maximum(jnp.max(raw, 0, keepdims=True), own)
        probs = jnp.exp2((raw - top) * factor).astype(BF16)
        own = jnp.exp2((own - top) * factor)
        both = dims(value, probs, 1, 0)
        total = both[head_dim : head_dim + 1] + own
        own_value = qkv[0, 2 * head_dim : 3 * head_dim, part].astype(F32)
        out[0, :, part] = ((both[:head_dim] + own * own_value) / total).astype(BF16)
        lse[0, :, part] = top + jnp.log2(total) * (1.0 / factor)


def split_rows(row):
    high = row.astype(BF16)
    rest = row - high.astype(F32)
    middle = rest.astype(BF16)
    low = (rest - middle.astype(F32)).astype(BF16)
    return [high, middle, low]


def backward_head(qkv, extra, pad, out, d_out, lse, grad, d_key, d_value, head_dim):
    count = qkv.shape[-1]
    scale = head_dim**-0.5
    factor = scale * LOG2E
    keys = qkv[0, head_dim : 2 * head_dim, :]
    keys_t = jnp.concatenate([keys, extra[1]], 0).T
    row = lax.broadcasted_iota(jnp.int32, (SPARE, count), 0)
    ones = jnp.where(row < 3, 1.0, 0.0).astype(BF16)
    value_t = jnp.concatenate([qkv[0, 2 * head_dim : 3 * head_dim, :], ones], 0).T

    for start in range(0, count, CHUNK):
        part = pl.ds(start, CHUNK)
        query = qkv[0, :head_dim, part]
        d_part = d_out[0, :, part]
        d_full = d_part.astype(F32)
        share = jnp.sum(d_full * out[0, :, part].astype(F32), 0, keepdims=True)
        row = lax.broadcasted_iota(jnp.int32, (SPARE, CHUNK), 0)

        def spread(values, at, base):
            for n, piece in enumerate(split_rows(values)):
                base = jnp.where(row == at + n, -piece.astype(F32), base)
            return base.astype(BF16)

        base = extra[0, :, part].astype(F32)
        query_x = jnp.concatenate([query, spread(lse[0, :, part], 5, base)], 0)
        d_part_x = jnp.concatenate([d_part, spread(share, 0, jnp.zeros_like(base))], 0)
        probs = jnp.exp2(dims(keys_t, query_x, 1, 0) * factor)
        d_scores = (probs * dims(value_t, d_part_x, 1, 0)).astype(BF16)
        probs_low = probs.astype(BF16)

        own_key = qkv[0, head_dim : 2 * head_dim, part].astype(F32)
        own_value = qkv[0, 2 * head_dim : 3 * head_dim, part].astype(F32)
        query_f = query.astype(F32)
        own = jnp.sum(query_f * own_key, 0, keepdims=True) + pad[:, part]
        own = jnp.exp2((own - lse[0, :, part]) * factor)
        own_ds = own * (jnp.sum(d_full * own_value, 0, keepdims=True) - share)

        grad[0, :head_dim, part] = (
            (dims(keys, d_scores, 1, 0) + own_ds * own_key) * scale
        ).astype(BF16)
        more_value = dims(d_part, probs_low, 1, 1)
        more_key = dims(query, d_scores, 1, 1)
        if start == 0:
            d_value[...] = more_value
            d_key[...] = more_key
        else:
            d_value[...] += more_value
            d_key[...] += more_key
        grad[0, head_dim : 2 * head_dim, part] = (own_ds * query_f).astype(BF16)
        grad[0, 2 * head_dim : 3 * head_dim, part] = (own * d_full).astype(BF16)
    for slot, total, factor_out in ((1, d_key, scale), (2, d_value, 1.0)):
        rows = pl.ds(slot * head_dim, head_dim)
        whole = total[...]
        grad[0, rows, :] = ((whole + grad[0, rows, :].astype(F32)) * factor_out).astype(BF16)
    grad[0, 3 * head_dim :, :] = jnp.zeros((SPARE, count), BF16)


def head_spec(rows, count):
    return pl.BlockSpec((1, rows, count), lambda h: (h, 0, 0))


def same(*shape):
    return pl.BlockSpec(shape, lambda h: (0,) * len(shape))


def spread_over(number, begin, end):
    inner = number - 2
    return [0] + [begin + n * (end - begin) // inner for n in range(inner)] + [HEADS - 1]


def run_stages(plan, when, chips):
    me, core = lax.axis_index("wide"), lax.axis_index("narrow")
    axes = chip_axes(chips)
    h = pl.program_id(0)

    @pl.when(h == 0)
    def _():
        greet(me, core, axes)

    for c in range(2):
        stages = plan(me, c, axes)
        for stage, step in zip(stages, spread_over(len(stages), *when)):
            @pl.when((core == c) & (h == step))
            def _(stage=stage):
                stage()


def attention(qkv, extra, pad, weights=(), chips=0, ident=None):
    rows, count = qkv.shape[1:]
    head_dim = (rows - SPARE) // 3
    n = len(weights)

    def body(*refs):
        (qkv_ref, extra_ref, pad_ref), ins = refs[:3], refs[3 : 3 + n]
        (out, lse), outs, sems = refs[3 + n : 5 + n], refs[5 + n : 5 + 2 * n], refs[5 + 2 * n :]
        if n:
            run_stages(
                lambda me, c, axes: gather_plan(ins, outs, sems, me, c, axes),
                GATHER_STEPS, chips,
            )
        forward_head(qkv_ref, extra_ref, pad_ref, out, lse, head_dim)

    return pl.pallas_call(
        body,
        grid=(HEADS,),
        out_shape=[
            jax.ShapeDtypeStruct((HEADS, head_dim, count), BF16),
            jax.ShapeDtypeStruct((HEADS, 1, count), F32),
        ]
        + [jax.ShapeDtypeStruct((chips,) + a.shape, a.dtype) for a in weights],
        in_specs=[head_spec(rows, count), same(2, SPARE, count), same(1, count)]
        + [same(*a.shape) for a in weights],
        out_specs=[head_spec(head_dim, count), head_spec(1, count)]
        + [pl.BlockSpec(memory_space=pl.ANY)] * n,
        scratch_shapes=gather_sems(chips, n) if n else [],
        compiler_params=pltpu.CompilerParams(
            vmem_limit_bytes=60 * 2**20, collective_id=ident, has_side_effects=n > 0
        ),
    )(qkv, extra, pad, *weights)


def attention_back(qkv, extra, pad, out, d_out, lse, grads=(), chips=0, ident=None):
    rows, count = qkv.shape[1:]
    head_dim = (rows - SPARE) // 3
    n = len(grads)

    def body(*refs):
        ins, refs = refs[:6], refs[6:]
        g_ins, grad, g_outs, rest = refs[:n], refs[n], refs[n + 1 : 2 * n + 1], refs[2 * n + 1 :]
        d_key, d_value = rest[:2]
        if n:
            parts, sems = scatter_parts(n, rest[2:])
            run_stages(
                lambda me, c, axes: scatter_plan(g_ins, g_outs, *parts, sems, me, c, axes),
                SCATTER_STEPS, chips,
            )
        backward_head(*ins, grad, d_key, d_value, head_dim)

    any_space = pl.BlockSpec(memory_space=pl.ANY)
    return pl.pallas_call(
        body,
        grid=(HEADS,),
        out_shape=[jax.ShapeDtypeStruct((HEADS, rows, count), BF16)]
        + [jax.ShapeDtypeStruct(a.shape[1:], F32) for a in grads],
        in_specs=[
            head_spec(rows, count),
            same(2, SPARE, count),
            same(1, count),
            head_spec(head_dim, count),
            head_spec(head_dim, count),
            head_spec(1, count),
        ]
        + [any_space] * n,
        out_specs=[head_spec(rows, count)] + [any_space] * n,
        scratch_shapes=[pltpu.VMEM((head_dim, count), F32)] * 2
        + (scatter_scratch(grads) if n else []),
        compiler_params=pltpu.CompilerParams(
            vmem_limit_bytes=60 * 2**20, collective_id=ident, has_side_effects=n > 0
        ),
    )(qkv, extra, pad, out, d_out, lse, *grads)


def masking_rows(seg, live):
    n = jnp.arange(SPARE)[:, None]
    seg, live = seg[None], live[None]
    group = n < SEGS
    query = jnp.where(group, seg == n, n == SEGS).astype(F32)
    keys = jnp.where(
        group,
        jnp.where(seg == n, 0.0, MASKED),
        jnp.where(
            n == SEGS,
            jnp.where(live > 0, 0.0, MASKED),
            jnp.where((n > SEGS) & (n < SEGS + 4), 1.0, 0.0),
        ),
    )
    return jnp.stack([query, keys]).astype(BF16), jnp.where(live > 0, MASKED, 0.0).astype(F32)


def norm(values):
    centred = values - jnp.mean(values, -1, keepdims=True)
    factor = lax.rsqrt(jnp.mean(centred * centred, -1, keepdims=True) + 1e-05)
    return centred * factor, factor


def norm_back(grad, normed, factor, gain):
    scaled = grad * gain
    inner = (
        scaled
        - jnp.mean(scaled, -1, keepdims=True)
        - normed * jnp.mean(scaled * normed, -1, keepdims=True)
    )
    return factor * inner, jnp.sum(grad * normed, 0), jnp.sum(grad, 0)


def gelu_pair(values):
    cdf = 0.5 * (1.0 + lax.erf(values * (1.0 / math.sqrt(2.0))))
    pdf = jnp.exp(-0.5 * values * values) * (1.0 / math.sqrt(2.0 * math.pi))
    return values * cdf, cdf + values * pdf


def row_sums(values):
    return jnp.sum(values.astype(F32), 0)


def widen(vector, width):
    return jnp.pad(vector, (0, width - vector.shape[0]))


def shards(
    chips,
    replicas,
    tokens,
    segment,
    keep,
    cotangent,
    gain_one,
    bias_one,
    w_query,
    b_query,
    w_key,
    w_value,
    b_value,
    w_out,
    b_out,
    gain_two,
    bias_two,
    w_hidden,
    b_hidden,
    w_proj,
    b_proj,
):
    own_copies = chips == HEADS and replicas == 2
    count, width = tokens.shape
    head_dim = width // HEADS
    hidden = w_hidden.shape[1] * chips
    vectors = (gain_one, bias_one, b_query, b_value, b_out, gain_two, bias_two, b_hidden, b_proj)
    packed = jnp.stack([widen(v, width) for v in vectors])
    packed = jnp.pad(packed, ((0, SPARE - len(vectors)), (0, 0)))

    if own_copies:
        first = jnp.concatenate([w_query.T, w_key.T, w_value.T, packed], 0)
        (first,) = gather([first], chips, 0)
        joined_t = first
        vector_rows = first[:, 3 * head_dim :, :]
    else:
        whole = [
            lax.all_gather(w.T, "wide", axis=0, tiled=True) for w in (w_query, w_key, w_value)
        ]
        whole = [w.reshape(HEADS, head_dim, width) for w in whole]
        whole.append(jnp.zeros((HEADS, SPARE, width), BF16))
        joined_t = jnp.concatenate(whole, 1)
        vector_rows = lax.all_gather(packed, "wide", axis=0, tiled=False)
        out_t, hidden_t, proj_t = [
            lax.all_gather(w.T, "wide", axis=0, tiled=False) for w in (w_out, w_hidden, w_proj)
        ]
    joined_t = joined_t.reshape(HEADS * (3 * head_dim + SPARE), width)
    gain_one_f, bias_one_f, b_query_f, b_value_f, b_out_f, gain_two_f, bias_two_f, b_hidden_f, b_proj_f = [
        vector_rows[:, n, : v.shape[0]].reshape(-1).astype(F32) for n, v in enumerate(vectors)
    ]

    live = keep[0]
    seg = segment[0]
    extra, pad = masking_rows(seg, live)

    x = tokens.astype(F32)
    xhat_one, factor_one = norm(x)
    h_one = (xhat_one * gain_one_f + bias_one_f).astype(BF16)
    block = 3 * head_dim + SPARE
    offsets = jnp.concatenate(
        [
            b_query_f.reshape(HEADS, head_dim),
            jnp.zeros((HEADS, head_dim), F32),
            b_value_f.reshape(HEADS, head_dim),
            jnp.zeros((HEADS, SPARE), F32),
        ],
        1,
    )
    row = jnp.arange(block)[None, :, None]
    qkv = dims(joined_t, h_one, 1, 1).reshape(HEADS, block, count) + offsets[:, :, None]
    qkv = jnp.where(row < 3 * head_dim, qkv, jnp.where(row == 3 * head_dim, 1.0, 0.0)).astype(BF16)
    if own_copies:
        o_t, lse, out_t, hidden_t, proj_t = attention(
            qkv, extra, pad, (w_out.T, w_hidden.T, w_proj.T), chips, 1
        )
    else:
        o_t, lse = attention(qkv, extra, pad)
    out_t = out_t.reshape(width, width)
    hidden_t = hidden_t.reshape(hidden, width)
    proj_t = proj_t.reshape(width, hidden)
    o_flat = o_t.reshape(width, count)
    x_one = x + dims(o_flat, out_t, 0, 1) + b_out_f
    xhat_two, factor_two = norm(x_one)
    h_two = (xhat_two * gain_two_f + bias_two_f).astype(BF16)
    upper = dims(h_two, hidden_t, 1, 1) + b_hidden_f
    act, slope = [v.astype(BF16) for v in gelu_pair(upper)]
    mixed = (x_one + dims(act, proj_t, 1, 1) + b_proj_f).astype(BF16)

    d_y = cotangent.astype(F32) * live.astype(F32)[:, None]
    d_m = d_y.astype(BF16)
    grad_proj = dims(d_m, act, 0, 0).astype(BF16)
    d_upper = (dims(d_m, proj_t, 1, 0) * slope.astype(F32)).astype(BF16)
    grad_hidden = dims(d_upper, h_two, 0, 0).astype(BF16)
    d_two, grad_gain_two, grad_bias_two = norm_back(
        dims(d_upper, hidden_t, 1, 0), xhat_two, factor_two, gain_two_f
    )
    d_x_one = d_y + d_two
    d_attn = d_x_one.astype(BF16)
    grad_out = dims(d_attn, o_flat, 0, 1).astype(BF16)
    d_o = dims(out_t, d_attn, 0, 1).astype(BF16).reshape(HEADS, head_dim, count)
    late = [
        g.reshape(chips, -1, g.shape[-1]) for g in (grad_out, grad_hidden, grad_proj)
    ]
    if own_copies:
        d_qkv, *late = attention_back(qkv, extra, pad, o_t, d_o, lse, late, chips, 2)
    else:
        (d_qkv,) = attention_back(qkv, extra, pad, o_t, d_o, lse)
    d_flat = d_qkv.reshape(HEADS * block, count)
    grad_qkv = dims(d_flat, h_one, 1, 0).reshape(HEADS, block, width)
    bias_sums = jnp.sum(d_qkv.astype(F32), -1)
    d_one, grad_gain_one, grad_bias_one = norm_back(
        dims(d_flat, joined_t, 0, 0), xhat_one, factor_one, gain_one_f
    )
    grad_tokens = d_x_one + d_one

    sums = (
        grad_gain_one,
        grad_bias_one,
        bias_sums[:, :head_dim].reshape(-1),
        bias_sums[:, 2 * head_dim : 3 * head_dim].reshape(-1),
        row_sums(d_attn),
        grad_gain_two,
        grad_bias_two,
        row_sums(d_upper),
        row_sums(d_m),
    )
    sums = jnp.stack(
        [jnp.pad(s.reshape(chips, -1), ((0, 0), (0, width - s.size // chips))) for s in sums], 1
    )
    sums = jnp.pad(sums, ((0, 0), (0, SPARE - sums.shape[1]), (0, 0)))
    part = width // chips
    if own_copies:
        early = jnp.concatenate([grad_qkv[:, : 3 * head_dim], sums], 1).astype(BF16)
        (early,) = scatter([early], 3)
        grads = [early[n * head_dim : (n + 1) * head_dim] for n in range(3)]
        vector_grads = early[3 * head_dim :]
    else:
        grads = [
            grad_qkv[:, n * head_dim : (n + 1) * head_dim].reshape(chips, part, width)
            for n in range(3)
        ]
        *grads, vector_grads = [
            lax.psum(
                lax.psum_scatter(g.astype(F32), "wide", scatter_dimension=0, tiled=False).astype(
                    BF16
                ),
                "narrow",
            ).astype(F32)
            for g in grads + [sums]
        ]
        late = [
            lax.psum(
                lax.psum_scatter(g.astype(F32), "wide", scatter_dimension=0, tiled=False).astype(
                    BF16
                ),
                "narrow",
            ).astype(F32)
            for g in late
        ]
    g_query, g_key, g_value = [g.T for g in grads]
    g_out, g_hidden, g_proj = [g.T for g in late]
    g_vec = [vector_grads[n, : v.shape[0]] for n, v in enumerate(vectors)]
    return (
        mixed, grad_tokens, g_vec[0], g_vec[1], g_query, g_vec[2], g_key, g_value, g_vec[3],
        g_out, g_vec[4], g_vec[5], g_vec[6], g_hidden, g_vec[7], g_proj, g_vec[8],
    )


def solution(mesh):
    both, wide = P(("wide", "narrow"), None), P("wide")
    weight = P(None, "wide")
    return jax.shard_map(
        functools.partial(shards, mesh.shape["wide"], mesh.shape["narrow"]),
        mesh=mesh,
        in_specs=(
            both, both, both, both, wide, wide, weight, wide, weight, weight, wide, weight, wide,
            wide, wide, weight, wide, weight, wide,
        ),
        out_specs=(
            both, both, wide, wide, weight, wide, weight, weight, wide, weight, wide, wide, wide,
            weight, wide, weight, wide,
        ),
        check_vma=False,
    )
```

```python
import functools
import itertools
import math

import jax
import jax.numpy as jnp
from jax import lax
from jax.experimental import pallas as pl
from jax.experimental.layout import Layout, with_layout_constraint
from jax.experimental.pallas import tpu as pltpu
from jax.sharding import PartitionSpec as P

HEADS = 16
F32 = jnp.float32
BF16 = jnp.bfloat16
MESH = pl.DeviceIdType.MESH
LOG2E = math.log2(math.e)
MASKED = -1e30
SPARE = 16
SEGS = 4
GATHER_STEPS = (2, HEADS + 3)
SCATTER_STEPS = (0, HEADS)
CHUNK = 512


def dims(left, right, a, b):
    return lax.dot_general(left, right, (((a,), (b,)), ((), ())), preferred_element_type=F32)


def chip_axes(chips):
    if chips == 16:
        return ((4, 4), (2, 2), (1, 2))
    return ((1, chips),)


def axis_orders(axes):
    if len(axes) == 3:
        return ((0, 1, 2), (2, 0, 1))
    return (tuple(range(len(axes))),) * 2


def place(me, axis):
    stride, size = axis
    return lax.rem(lax.div(me, stride), size)


def peer(me, axis, step):
    stride, size = axis
    mine = place(me, axis)
    other = lax.rem(mine + step, size)
    return me + (other - mine) * stride


def greet(me, core, axes):
    barrier = pltpu.get_barrier_semaphore()
    count = 1
    pl.semaphore_signal(barrier, 1, device_id=(me, 1 - core), device_id_type=MESH)
    for axis in axes:
        for step in range(1, axis[1]):
            pl.semaphore_signal(
                barrier, 1, device_id=(peer(me, axis, step), core), device_id_type=MESH
            )
            count += 1
    pl.semaphore_wait(barrier, count)


def moved(me, axes, order, steps, sign):
    for a, step in zip(order, steps):
        size = axes[a][1]
        if step:
            other = peer(me, axes[a], step if sign > 0 else size - step)
            me = me + (other - me)
    return me


def grid_of(axes, order):
    return [range(axes[a][1]) for a in order]


def slots_of(axes, order):
    slots = {}
    for k in range(len(order)):
        for steps in itertools.product(*grid_of(axes, order[: k + 1])):
            if steps[-1]:
                slots[steps] = len(slots)
    return slots


def half(ref, block, c):
    width = ref.shape[-1] // 2
    return ref.at[block, :, pl.ds(c * width, width)]


def flat_half(ref, c):
    width = ref.shape[-1] // 2
    return ref.at[:, pl.ds(c * width, width)]


def gather_plan(ins, outs, sems, me, c, axes):
    order = axis_orders(axes)[c]
    send, recv, pass_send, pass_recv, own = sems
    arrays = len(outs)
    slots = slots_of(axes, order)

    def block_of(steps):
        return moved(me, axes, order, steps, -1)

    def message(steps):
        before = steps[:-1]
        target = moved(me, axes, order[len(before) :], steps[-1:], 1)
        block = block_of(before)
        fresh = not any(before)
        return [
            pltpu.make_async_remote_copy(
                flat_half(src, c) if fresh else half(dst, block, c),
                half(dst, block, c),
                send.at[slots[steps] * arrays + k],
                recv.at[slots[steps] * arrays + k],
                device_id=(target, c), device_id_type=MESH,
            )
            for k, (src, dst) in enumerate(zip(ins, outs))
        ]

    def send_on(steps):
        for k in range(len(steps), len(order)):
            lead = steps + (0,) * (k - len(steps))
            for step in range(1, axes[order[k]][1]):
                for copy in message(lead + (step,)):
                    copy.start()

    def hand_over(steps):
        block = block_of(steps)
        return [
            pltpu.make_async_remote_copy(
                half(dst, block, c), half(dst, block, c),
                pass_send.at[slots[steps] * arrays + k], pass_recv.at[slots[steps] * arrays + k],
                device_id=(me, 1 - c), device_id_type=MESH,
            )
            for k, dst in enumerate(outs)
        ]

    def keep_own():
        return [pltpu.make_async_copy(s, d.at[me], own.at[k]) for k, (s, d) in enumerate(zip(ins, outs))]

    def first():
        send_on(())
        for copy in keep_own():
            copy.start()

    def arrive(steps):
        def run():
            for copy in message(steps):
                copy.wait_recv()
            send_on(steps)
            for copy in hand_over(steps):
                copy.start()
        return run

    def last():
        for copy in keep_own():
            copy.wait()
        for steps in slots:
            for copy in message(steps):
                copy.wait_send()
            for copy in hand_over(steps):
                copy.wait_send()
        other = axis_orders(axes)[1 - c]
        other_slots = slots_of(axes, other)
        for steps, slot in other_slots.items():
            block = moved(me, axes, other, steps, -1)
            for k, dst in enumerate(outs):
                n = slot * arrays + k
                pltpu.make_async_remote_copy(
                    half(dst, block, 1 - c), half(dst, block, 1 - c),
                    pass_send.at[n], pass_recv.at[n],
                    device_id=(me, 1 - c), device_id_type=MESH,
                ).wait_recv()

    def cost(steps):
        return (sum(1 for s in steps if s), len(steps), steps)

    return [first] + [arrive(steps) for steps in sorted(slots, key=cost)] + [last]


def gather_sems(chips, arrays):
    total = (chips - 1) * arrays
    return [pltpu.SemaphoreType.DMA((total,)) for _ in range(4)] + [
        pltpu.SemaphoreType.DMA((arrays,))
    ]


def gather_kernel(chips, arrays, *refs):
    ins, outs, sems = refs[:arrays], refs[arrays : 2 * arrays], refs[2 * arrays :]
    me, core = lax.axis_index("wide"), lax.axis_index("narrow")
    axes = chip_axes(chips)
    greet(me, core, axes)
    for c in range(2):
        @pl.when(core == c)
        def _():
            for stage in gather_plan(ins, outs, sems, me, c, axes):
                stage()


def gather(arrays, chips, ident):
    vm = pl.BlockSpec(memory_space=pltpu.VMEM)
    return pl.pallas_call(
        functools.partial(gather_kernel, chips, len(arrays)),
        out_shape=[jax.ShapeDtypeStruct((chips,) + a.shape, a.dtype) for a in arrays],
        in_specs=[vm] * len(arrays),
        out_specs=[pl.BlockSpec(memory_space=pl.ANY)] * len(arrays),
        scratch_shapes=gather_sems(chips, len(arrays)),
        compiler_params=pltpu.CompilerParams(collective_id=ident, has_side_effects=True),
    )(*arrays)


def scatter_plan(ins, outs, accs, halves, landed, results, sems, me, c, axes):
    order = axis_orders(axes)[c]
    send, recv, swap_send, swap_recv, own, out_sem, last_send, last_recv = sems
    arrays = len(ins)
    slots = slots_of(axes, order)
    depth = len(order)

    def all_steps(number):
        steps = itertools.product(*grid_of(axes, order[:number]))
        return sorted(steps, key=lambda t: (-sum(1 for s in t if s), [-s for s in reversed(t)]))

    def owner(steps):
        return moved(me, axes, order, steps, 1)

    whole = all_steps(depth)

    def swap(steps, core):
        there = axis_orders(axes)[core]
        names = all_steps_of(there)
        n = names.index(steps)
        block = moved(me, axes, there, steps, 1)
        return [
            pltpu.make_async_remote_copy(
                half(ins[k], block, core), halves[k].at[block],
                swap_send.at[n * arrays + k], swap_recv.at[n * arrays + k],
                device_id=(me, 1 - c), device_id_type=MESH,
            )
            for k in range(arrays)
        ]

    def all_steps_of(there):
        steps = itertools.product(*grid_of(axes, there))
        return sorted(steps, key=lambda t: (-sum(1 for s in t if s), [-s for s in reversed(t)]))

    def load(steps):
        block = owner(steps)
        n = whole.index(steps)
        return [
            pltpu.make_async_copy(half(ins[k], block, c), accs[k].at[block], own.at[n * arrays + k])
            for k in range(arrays)
        ]

    def message(steps):
        block = owner(steps)
        target = moved(me, axes, order[len(steps) - 1 :], steps[-1:], 1)
        slot = slots[steps]
        return [
            pltpu.make_async_remote_copy(
                accs[k].at[block], landed[k].at[slot],
                send.at[slot * arrays + k], recv.at[slot * arrays + k],
                device_id=(target, c), device_id_type=MESH,
            )
            for k in range(arrays)
        ]

    def send_on(steps):
        if steps and steps[-1]:
            for copy in message(steps):
                copy.start()

    def first():
        for steps in all_steps_of(axis_orders(axes)[1 - c]):
            for copy in swap(steps, 1 - c):
                copy.start()
        for steps in whole:
            for copy in load(steps):
                copy.start()

    def add_pair(steps):
        def run():
            for copy in load(steps):
                copy.wait()
            for copy in swap(steps, c):
                copy.wait_recv()
            block = owner(steps)
            for k in range(arrays):
                accs[k][block] = (
                    accs[k][block].astype(F32) + halves[k][block].astype(F32)
                ).astype(BF16)
            send_on(steps)
        return run

    def add(steps):
        def run():
            got = [steps + (s,) for s in range(1, axes[order[len(steps)]][1])]
            for came in got:
                for copy in message(came):
                    copy.wait_recv()
            block = owner(steps)
            for k in range(arrays):
                total = accs[k][block].astype(F32)
                for came in got:
                    total = total + landed[k][slots[came]].astype(F32)
                if steps:
                    accs[k][block] = total.astype(BF16)
                else:
                    width = total.shape[-1]
                    results[k][:, pl.ds(c * width, width)] = total
            if steps:
                send_on(steps)
            else:
                for copy in finals(c):
                    copy.start()
        return run

    def finals(core):
        return [
            pltpu.make_async_remote_copy(
                flat_half(results[k], core), flat_half(results[k], core),
                last_send.at[k], last_recv.at[k],
                device_id=(me, 1 - c), device_id_type=MESH,
            )
            for k in range(arrays)
        ]

    def last():
        for steps in slots:
            for copy in message(steps):
                copy.wait_send()
        for steps in all_steps_of(axis_orders(axes)[1 - c]):
            for copy in swap(steps, 1 - c):
                copy.wait_send()
        outgoing = [pltpu.make_async_copy(results[k], outs[k], out_sem.at[k]) for k in range(arrays)]
        for copy in finals(c):
            copy.wait_send()
        for copy, out in zip(finals(1 - c), outgoing):
            copy.wait_recv()
            out.start()
        for out in outgoing:
            out.wait()

    def settle(steps):
        def run():
            add_pair(steps + (0,))()
            add(steps)()
        return run

    events = [first] + [add_pair(steps) for steps in whole if steps[-1]]
    events += [settle(steps) for steps in all_steps(depth - 1)]
    for number in reversed(range(depth - 1)):
        events += [add(steps) for steps in all_steps(number)]
    return events + [last]


def scatter_scratch(arrays):
    chips = arrays[0].shape[0]
    number = len(arrays)
    scratch = []
    for rows in (chips, chips, chips - 1):
        scratch += [pltpu.VMEM((rows, a.shape[1], a.shape[2] // 2), BF16) for a in arrays]
    scratch += [pltpu.VMEM(a.shape[1:], F32) for a in arrays]
    dma = pltpu.SemaphoreType.DMA
    sizes = (chips - 1,) * 2 + (chips,) * 3 + (1,) * 3
    return scratch + [dma((n * number,)) for n in sizes]


def scatter_parts(arrays, refs):
    parts = [refs[n * arrays : (n + 1) * arrays] for n in range(4)]
    return parts, refs[4 * arrays :]


def scatter_kernel(chips, arrays, *refs):
    ins, outs = refs[:arrays], refs[arrays : 2 * arrays]
    parts, sems = scatter_parts(arrays, refs[2 * arrays :])
    me, core = lax.axis_index("wide"), lax.axis_index("narrow")
    axes = chip_axes(chips)
    greet(me, core, axes)
    for c in range(2):
        @pl.when(core == c)
        def _():
            for stage in scatter_plan(ins, outs, *parts, sems, me, c, axes):
                stage()


def scatter(arrays, ident):
    any_space = pl.BlockSpec(memory_space=pl.ANY)
    return pl.pallas_call(
        functools.partial(scatter_kernel, arrays[0].shape[0], len(arrays)),
        out_shape=[jax.ShapeDtypeStruct(a.shape[1:], F32) for a in arrays],
        in_specs=[any_space] * len(arrays),
        out_specs=[any_space] * len(arrays),
        scratch_shapes=scatter_scratch(arrays),
        compiler_params=pltpu.CompilerParams(
            collective_id=ident, has_side_effects=True, vmem_limit_bytes=60 * 2**20
        ),
    )(*arrays)


def forward_head(qkv, extra, pad, out, lse, head_dim):
    count = qkv.shape[-1]
    factor = head_dim**-0.5 * LOG2E
    keys = jnp.concatenate([qkv[0, head_dim : 2 * head_dim, :], extra[1]], 0).T
    value = qkv[0, 2 * head_dim : 3 * head_dim + SPARE, :]

    for start in range(0, count, CHUNK):
        part = pl.ds(start, CHUNK)
        query = qkv[0, :head_dim, part]
        own_key = qkv[0, head_dim : 2 * head_dim, part]
        own = jnp.sum(query.astype(F32) * own_key.astype(F32), 0, keepdims=True) + pad[:, part]
        raw = dims(keys, jnp.concatenate([query, extra[0, :, part]], 0), 1, 0)
        top = jnp.maximum(jnp.max(raw, 0, keepdims=True), own)
        probs = jnp.exp2((raw - top) * factor).astype(BF16)
        own = jnp.exp2((own - top) * factor)
        both = dims(value, probs, 1, 0)
        total = both[head_dim : head_dim + 1] + own
        own_value = qkv[0, 2 * head_dim : 3 * head_dim, part].astype(F32)
        out[0, :, part] = ((both[:head_dim] + own * own_value) / total).astype(BF16)
        lse[0, :, part] = top + jnp.log2(total) * (1.0 / factor)


def split_rows(row):
    high = row.astype(BF16)
    rest = row - high.astype(F32)
    middle = rest.astype(BF16)
    low = (rest - middle.astype(F32)).astype(BF16)
    return [high, middle, low]


def backward_head(qkv, extra, pad, out, d_out, lse, grad, d_key, d_value, head_dim):
    count = qkv.shape[-1]
    scale = head_dim**-0.5
    factor = scale * LOG2E
    keys = qkv[0, head_dim : 2 * head_dim, :]
    keys_t = jnp.concatenate([keys, extra[1]], 0).T
    row = lax.broadcasted_iota(jnp.int32, (SPARE, count), 0)
    ones = jnp.where(row < 3, 1.0, 0.0).astype(BF16)
    value_t = jnp.concatenate([qkv[0, 2 * head_dim : 3 * head_dim, :], ones], 0).T

    for start in range(0, count, CHUNK):
        part = pl.ds(start, CHUNK)
        query = qkv[0, :head_dim, part]
        d_part = d_out[0, :, part]
        d_full = d_part.astype(F32)
        share = jnp.sum(d_full * out[0, :, part].astype(F32), 0, keepdims=True)
        row = lax.broadcasted_iota(jnp.int32, (SPARE, CHUNK), 0)

        def spread(values, at, base):
            for n, piece in enumerate(split_rows(values)):
                base = jnp.where(row == at + n, -piece.astype(F32), base)
            return base.astype(BF16)

        base = extra[0, :, part].astype(F32)
        query_x = jnp.concatenate([query, spread(lse[0, :, part], 5, base)], 0)
        d_part_x = jnp.concatenate([d_part, spread(share, 0, jnp.zeros_like(base))], 0)
        probs = jnp.exp2(dims(keys_t, query_x, 1, 0) * factor)
        d_scores = (probs * dims(value_t, d_part_x, 1, 0)).astype(BF16)
        probs_low = probs.astype(BF16)

        own_key = qkv[0, head_dim : 2 * head_dim, part].astype(F32)
        own_value = qkv[0, 2 * head_dim : 3 * head_dim, part].astype(F32)
        query_f = query.astype(F32)
        own = jnp.sum(query_f * own_key, 0, keepdims=True) + pad[:, part]
        own = jnp.exp2((own - lse[0, :, part]) * factor)
        own_ds = own * (jnp.sum(d_full * own_value, 0, keepdims=True) - share)

        grad[0, :head_dim, part] = (
            (dims(keys, d_scores, 1, 0) + own_ds * own_key) * scale
        ).astype(BF16)
        more_value = dims(d_part, probs_low, 1, 1)
        more_key = dims(query, d_scores, 1, 1)
        if start == 0:
            d_value[...] = more_value
            d_key[...] = more_key
        else:
            d_value[...] += more_value
            d_key[...] += more_key
        grad[0, head_dim : 2 * head_dim, part] = (own_ds * query_f).astype(BF16)
        grad[0, 2 * head_dim : 3 * head_dim, part] = (own * d_full).astype(BF16)
    for slot, total, factor_out in ((1, d_key, scale), (2, d_value, 1.0)):
        rows = pl.ds(slot * head_dim, head_dim)
        whole = total[...]
        grad[0, rows, :] = ((whole + grad[0, rows, :].astype(F32)) * factor_out).astype(BF16)
    grad[0, 3 * head_dim :, :] = jnp.zeros((SPARE, count), BF16)


def head_spec(rows, count):
    return pl.BlockSpec((1, rows, count), lambda h: (h, 0, 0))


def same(*shape):
    return pl.BlockSpec(shape, lambda h: (0,) * len(shape))


def spread_over(number, begin, end):
    inner = number - 2
    steps = [begin + n * (end - begin) // inner for n in range(inner)]
    return [0] + [min(step, HEADS - 1) for step in steps] + [HEADS - 1]


def run_stages(plan, when, chips):
    me, core = lax.axis_index("wide"), lax.axis_index("narrow")
    axes = chip_axes(chips)
    h = pl.program_id(0)

    @pl.when(h == 0)
    def _():
        greet(me, core, axes)

    for c in range(2):
        stages = plan(me, c, axes)
        for stage, step in zip(stages, spread_over(len(stages), *when)):
            @pl.when((core == c) & (h == step))
            def _(stage=stage):
                stage()


def attention(qkv, extra, pad, weights=(), chips=0, ident=None):
    rows, count = qkv.shape[1:]
    head_dim = (rows - SPARE) // 3
    n = len(weights)

    def body(*refs):
        (qkv_ref, extra_ref, pad_ref), ins = refs[:3], refs[3 : 3 + n]
        (out, lse), outs, sems = refs[3 + n : 5 + n], refs[5 + n : 5 + 2 * n], refs[5 + 2 * n :]
        if n:
            run_stages(
                lambda me, c, axes: gather_plan(ins, outs, sems, me, c, axes),
                GATHER_STEPS, chips,
            )
        forward_head(qkv_ref, extra_ref, pad_ref, out, lse, head_dim)

    return pl.pallas_call(
        body,
        grid=(HEADS,),
        out_shape=[
            jax.ShapeDtypeStruct((HEADS, head_dim, count), BF16),
            jax.ShapeDtypeStruct((HEADS, 1, count), F32),
        ]
        + [jax.ShapeDtypeStruct((chips,) + a.shape, a.dtype) for a in weights],
        in_specs=[head_spec(rows, count), same(2, SPARE, count), same(1, count)]
        + [same(*a.shape) for a in weights],
        out_specs=[head_spec(head_dim, count), head_spec(1, count)]
        + [pl.BlockSpec(memory_space=pl.ANY)] * n,
        scratch_shapes=gather_sems(chips, n) if n else [],
        compiler_params=pltpu.CompilerParams(
            vmem_limit_bytes=60 * 2**20, collective_id=ident, has_side_effects=n > 0
        ),
    )(qkv, extra, pad, *weights)


def attention_back(qkv, extra, pad, out, d_out, lse, grads=(), chips=0, ident=None):
    rows, count = qkv.shape[1:]
    head_dim = (rows - SPARE) // 3
    n = len(grads)

    def body(*refs):
        ins, refs = refs[:6], refs[6:]
        g_ins, grad, g_outs, rest = refs[:n], refs[n], refs[n + 1 : 2 * n + 1], refs[2 * n + 1 :]
        d_key, d_value = rest[:2]
        if n:
            parts, sems = scatter_parts(n, rest[2:])
            run_stages(
                lambda me, c, axes: scatter_plan(g_ins, g_outs, *parts, sems, me, c, axes),
                SCATTER_STEPS, chips,
            )
        backward_head(*ins, grad, d_key, d_value, head_dim)

    any_space = pl.BlockSpec(memory_space=pl.ANY)
    return pl.pallas_call(
        body,
        grid=(HEADS,),
        out_shape=[jax.ShapeDtypeStruct((HEADS, rows, count), BF16)]
        + [jax.ShapeDtypeStruct(a.shape[1:], F32) for a in grads],
        in_specs=[
            head_spec(rows, count),
            same(2, SPARE, count),
            same(1, count),
            head_spec(head_dim, count),
            head_spec(head_dim, count),
            head_spec(1, count),
        ]
        + [any_space] * n,
        out_specs=[head_spec(rows, count)] + [any_space] * n,
        scratch_shapes=[pltpu.VMEM((head_dim, count), F32)] * 2
        + (scatter_scratch(grads) if n else []),
        compiler_params=pltpu.CompilerParams(
            vmem_limit_bytes=60 * 2**20, collective_id=ident, has_side_effects=n > 0
        ),
    )(qkv, extra, pad, out, d_out, lse, *grads)


def masking_rows(seg, live):
    n = jnp.arange(SPARE)[:, None]
    seg, live = seg[None], live[None]
    group = n < SEGS
    query = jnp.where(group, seg == n, n == SEGS).astype(F32)
    keys = jnp.where(
        group,
        jnp.where(seg == n, 0.0, MASKED),
        jnp.where(
            n == SEGS,
            jnp.where(live > 0, 0.0, MASKED),
            jnp.where((n > SEGS) & (n < SEGS + 4), 1.0, 0.0),
        ),
    )
    return jnp.stack([query, keys]).astype(BF16), jnp.where(live > 0, MASKED, 0.0).astype(F32)


def norm(values):
    centred = values - jnp.mean(values, -1, keepdims=True)
    factor = lax.rsqrt(jnp.mean(centred * centred, -1, keepdims=True) + 1e-05)
    return centred * factor, factor


def norm_back(grad, normed, factor, gain):
    scaled = grad * gain
    inner = (
        scaled
        - jnp.mean(scaled, -1, keepdims=True)
        - normed * jnp.mean(scaled * normed, -1, keepdims=True)
    )
    return factor * inner, jnp.sum(grad * normed, 0), jnp.sum(grad, 0)


def gelu_pair(values):
    cdf = 0.5 * (1.0 + lax.erf(values * (1.0 / math.sqrt(2.0))))
    pdf = jnp.exp(-0.5 * values * values) * (1.0 / math.sqrt(2.0 * math.pi))
    return values * cdf, cdf + values * pdf


def by_rows(values):
    return with_layout_constraint(values, Layout((0, 1)))


def row_sums(values):
    return dims(jnp.ones((8, values.shape[0]), BF16), values, 1, 0)[0]


def widen(vector, width):
    return jnp.pad(vector, (0, width - vector.shape[0]))


def shards(
    chips,
    replicas,
    tokens,
    segment,
    keep,
    cotangent,
    gain_one,
    bias_one,
    w_query,
    b_query,
    w_key,
    w_value,
    b_value,
    w_out,
    b_out,
    gain_two,
    bias_two,
    w_hidden,
    b_hidden,
    w_proj,
    b_proj,
):
    own_copies = chips == HEADS and replicas == 2
    count, width = tokens.shape
    head_dim = width // HEADS
    hidden = w_hidden.shape[1] * chips
    vectors = (gain_one, bias_one, b_query, b_value, b_out, gain_two, bias_two, b_hidden, b_proj)
    packed = jnp.stack([widen(v, width) for v in vectors])
    packed = jnp.pad(packed, ((0, SPARE - len(vectors)), (0, 0)))

    if own_copies:
        first = jnp.concatenate([w_query.T, w_key.T, w_value.T, packed], 0)
        (first,) = gather([first], chips, 0)
        joined_t = first
        vector_rows = first[:, 3 * head_dim :, :]
    else:
        whole = [
            lax.all_gather(w.T, "wide", axis=0, tiled=True) for w in (w_query, w_key, w_value)
        ]
        whole = [w.reshape(HEADS, head_dim, width) for w in whole]
        whole.append(jnp.zeros((HEADS, SPARE, width), BF16))
        joined_t = jnp.concatenate(whole, 1)
        vector_rows = lax.all_gather(packed, "wide", axis=0, tiled=False)
        out_t, hidden_t, proj_t = [
            lax.all_gather(w.T, "wide", axis=0, tiled=False) for w in (w_out, w_hidden, w_proj)
        ]
    joined_t = joined_t.reshape(HEADS * (3 * head_dim + SPARE), width)
    gain_one_f, bias_one_f, b_query_f, b_value_f, b_out_f, gain_two_f, bias_two_f, b_hidden_f, b_proj_f = [
        vector_rows[:, n, : v.shape[0]].reshape(-1).astype(F32) for n, v in enumerate(vectors)
    ]

    live = keep[0]
    seg = segment[0]
    extra, pad = masking_rows(seg, live)

    x = by_rows(tokens).astype(F32)
    xhat_one, factor_one = norm(x)
    h_one = lax.optimization_barrier((xhat_one * gain_one_f + bias_one_f).astype(BF16))
    block = 3 * head_dim + SPARE
    offsets = jnp.concatenate(
        [
            b_query_f.reshape(HEADS, head_dim),
            jnp.zeros((HEADS, head_dim), F32),
            b_value_f.reshape(HEADS, head_dim),
            jnp.zeros((HEADS, SPARE), F32),
        ],
        1,
    )
    row = jnp.arange(block)[None, :, None]
    qkv = dims(joined_t, h_one, 1, 1).reshape(HEADS, block, count) + offsets[:, :, None]
    qkv = jnp.where(row < 3 * head_dim, qkv, jnp.where(row == 3 * head_dim, 1.0, 0.0)).astype(BF16)
    if own_copies:
        o_t, lse, out_t, hidden_t, proj_t = attention(
            qkv, extra, pad, (w_out.T, w_hidden.T, w_proj.T), chips, 1
        )
    else:
        o_t, lse = attention(qkv, extra, pad)
    out_t = out_t.reshape(width, width)
    hidden_t = hidden_t.reshape(hidden, width)
    proj_t = proj_t.reshape(width, hidden)
    o_flat = o_t.reshape(width, count)
    x_one = by_rows(x + dims(o_flat, out_t, 0, 1) + b_out_f)
    xhat_two, factor_two = norm(x_one)
    h_two = lax.optimization_barrier((xhat_two * gain_two_f + bias_two_f).astype(BF16))
    upper = dims(h_two, hidden_t, 1, 1) + b_hidden_f
    act, slope = [v.astype(BF16) for v in gelu_pair(upper)]
    mixed = (x_one + dims(act, proj_t, 1, 1) + b_proj_f).astype(BF16)

    d_y = by_rows(cotangent).astype(F32) * live.astype(F32)[:, None]
    d_m = d_y.astype(BF16)
    grad_proj = dims(d_m, act, 0, 0).astype(BF16)
    d_upper = (dims(d_m, proj_t, 1, 0) * slope.astype(F32)).astype(BF16)
    grad_hidden = dims(d_upper, h_two, 0, 0).astype(BF16)
    d_two, grad_gain_two, grad_bias_two = norm_back(
        dims(d_upper, hidden_t, 1, 0), xhat_two, factor_two, gain_two_f
    )
    d_x_one = by_rows(d_y + d_two)
    d_attn = d_x_one.astype(BF16)
    grad_out = dims(d_attn, o_flat, 0, 1).astype(BF16)
    d_o = dims(out_t, d_attn, 0, 1).astype(BF16).reshape(HEADS, head_dim, count)
    late = [
        g.reshape(chips, -1, g.shape[-1]) for g in (grad_out, grad_hidden, grad_proj)
    ]
    if own_copies:
        d_qkv, *late = attention_back(qkv, extra, pad, o_t, d_o, lse, late, chips, 2)
    else:
        (d_qkv,) = attention_back(qkv, extra, pad, o_t, d_o, lse)
    d_flat = d_qkv.reshape(HEADS * block, count)
    grad_qkv = dims(d_flat, h_one, 1, 0).reshape(HEADS, block, width)
    bias_sums = dims(jnp.ones((8, count), BF16), d_flat, 1, 1)[0].reshape(HEADS, block)
    d_one, grad_gain_one, grad_bias_one = norm_back(
        dims(d_flat, joined_t, 0, 0), xhat_one, factor_one, gain_one_f
    )
    grad_tokens = d_x_one + d_one

    part = width // chips
    sums = jnp.stack([
        grad_gain_one,
        grad_bias_one,
        bias_sums[:, :head_dim].reshape(-1),
        bias_sums[:, 2 * head_dim : 3 * head_dim].reshape(-1),
        row_sums(d_attn),
        grad_gain_two,
        grad_bias_two,
        row_sums(d_m),
    ])
    sums = sums.reshape(-1, chips, part).transpose(1, 0, 2)
    more = row_sums(d_upper).reshape(chips, -1, part)
    sums = jnp.concatenate([sums, more], 1)
    sums = jnp.pad(sums, ((0, 0), (0, SPARE - sums.shape[1]), (0, width - part)))
    if own_copies:
        early = jnp.concatenate([grad_qkv[:, : 3 * head_dim], sums], 1).astype(BF16)
        (early,) = scatter([early], 3)
        grads = [early[n * head_dim : (n + 1) * head_dim] for n in range(3)]
        vector_grads = early[3 * head_dim :]
    else:
        grads = [
            grad_qkv[:, n * head_dim : (n + 1) * head_dim].reshape(chips, part, width)
            for n in range(3)
        ]
        *grads, vector_grads = [
            lax.psum(
                lax.psum_scatter(g.astype(F32), "wide", scatter_dimension=0, tiled=False).astype(
                    BF16
                ),
                "narrow",
            ).astype(F32)
            for g in grads + [sums]
        ]
        late = [
            lax.psum(
                lax.psum_scatter(g.astype(F32), "wide", scatter_dimension=0, tiled=False).astype(
                    BF16
                ),
                "narrow",
            ).astype(F32)
            for g in late
        ]
    g_query, g_key, g_value = [g.T for g in grads]
    g_out, g_hidden, g_proj = [g.T for g in late]
    g_vec = [vector_grads[n, :part] for n in range(8)]
    ratio = hidden // width
    g_vec.insert(7, vector_grads[8 : 8 + ratio, :part].reshape(-1))
    return (
        mixed, grad_tokens, g_vec[0], g_vec[1], g_query, g_vec[2], g_key, g_value, g_vec[3],
        g_out, g_vec[4], g_vec[5], g_vec[6], g_hidden, g_vec[7], g_proj, g_vec[8],
    )


def solution(mesh):
    both, wide = P(("wide", "narrow"), None), P("wide")
    weight = P(None, "wide")
    return jax.shard_map(
        functools.partial(shards, mesh.shape["wide"], mesh.shape["narrow"]),
        mesh=mesh,
        in_specs=(
            both, both, both, both, wide, wide, weight, wide, weight, weight, wide, weight, wide,
            wide, wide, weight, wide, weight, wide,
        ),
        out_specs=(
            both, both, wide, wide, weight, wide, weight, weight, wide, weight, wide, wide, wide,
            weight, wide, weight, wide,
        ),
        check_vma=False,
    )
```

```python
import functools
import itertools
import math

import jax
import jax.numpy as jnp
from jax import lax
from jax.experimental import pallas as pl
from jax.experimental.layout import Layout, with_layout_constraint
from jax.experimental.pallas import tpu as pltpu
from jax.sharding import PartitionSpec as P

HEADS = 16
F32 = jnp.float32
BF16 = jnp.bfloat16
MESH = pl.DeviceIdType.MESH
LOG2E = math.log2(math.e)
MASKED = -1e30
SPARE = 16
SEGS = 4
CHUNK = 512


def dims(left, right, a, b):
    return lax.dot_general(left, right, (((a,), (b,)), ((), ())), preferred_element_type=F32)


def chip_axes(chips):
    if chips == 16:
        return ((4, 4), (2, 2), (1, 2))
    return ((1, chips),)


def axis_orders(axes):
    if len(axes) == 3:
        return ((0, 1, 2), (2, 0, 1))
    return (tuple(range(len(axes))),) * 2


def place(me, axis):
    stride, size = axis
    return lax.rem(lax.div(me, stride), size)


def peer(me, axis, step):
    stride, size = axis
    mine = place(me, axis)
    other, bit = 0, 1
    while bit < size:
        digit = lax.rem(lax.div(mine, bit), 2)
        other = other + bit * ((1 - digit) if step & bit else digit)
        bit *= 2
    return me + (other - mine) * stride


def greet(me, core, axes):
    barrier = pltpu.get_barrier_semaphore()
    count = 1
    pl.semaphore_signal(barrier, 1, device_id=(me, 1 - core), device_id_type=MESH)
    for axis in axes:
        for step in range(1, axis[1]):
            pl.semaphore_signal(
                barrier, 1, device_id=(peer(me, axis, step), core), device_id_type=MESH
            )
            count += 1
    pl.semaphore_wait(barrier, count)


def moved(me, axes, order, steps):
    for a, step in zip(order, steps):
        if step:
            me = peer(me, axes[a], step)
    return me


def grid_of(axes, order):
    return [range(axes[a][1]) for a in order]


def slots_of(axes, order):
    slots = {}
    for k in range(len(order)):
        for steps in itertools.product(*grid_of(axes, order[: k + 1])):
            if steps[-1]:
                slots[steps] = len(slots)
    return slots


def half(ref, block, c):
    width = ref.shape[-1] // 2
    return ref.at[block, :, pl.ds(c * width, width)]


def flat_half(ref, c):
    width = ref.shape[-1] // 2
    return ref.at[:, pl.ds(c * width, width)]


def gather_plan(ins, outs, sems, me, c, axes):
    order = axis_orders(axes)[c]
    send, recv, pass_send, pass_recv, own = sems
    arrays = len(outs)
    slots = slots_of(axes, order)

    def block_of(steps):
        return moved(me, axes, order, steps)

    def message(steps):
        before = steps[:-1]
        target = moved(me, axes, order[len(before) :], steps[-1:])
        block = block_of(before)
        fresh = not any(before)
        return [
            pltpu.make_async_remote_copy(
                flat_half(src, c) if fresh else half(dst, block, c),
                half(dst, block, c),
                send.at[slots[steps] * arrays + k],
                recv.at[slots[steps] * arrays + k],
                device_id=(target, c), device_id_type=MESH,
            )
            for k, (src, dst) in enumerate(zip(ins, outs))
        ]

    def send_on(steps):
        for k in range(len(steps), len(order)):
            lead = steps + (0,) * (k - len(steps))
            for step in reversed(range(1, axes[order[k]][1])):
                for copy in message(lead + (step,)):
                    copy.start()

    def hand_over(steps):
        block = block_of(steps)
        return [
            pltpu.make_async_remote_copy(
                half(dst, block, c), half(dst, block, c),
                pass_send.at[slots[steps] * arrays + k], pass_recv.at[slots[steps] * arrays + k],
                device_id=(me, 1 - c), device_id_type=MESH,
            )
            for k, dst in enumerate(outs)
        ]

    def keep_own():
        return [pltpu.make_async_copy(s, d.at[me], own.at[k]) for k, (s, d) in enumerate(zip(ins, outs))]

    def first():
        send_on(())
        for copy in keep_own():
            copy.start()

    def arrive(steps):
        def run():
            for copy in message(steps):
                copy.wait_recv()
            send_on(steps)
            for copy in hand_over(steps):
                copy.start()
        return run

    def last():
        for copy in keep_own():
            copy.wait()
        for steps in slots:
            for copy in message(steps):
                copy.wait_send()
            for copy in hand_over(steps):
                copy.wait_send()
        other = axis_orders(axes)[1 - c]
        other_slots = slots_of(axes, other)
        for steps, slot in other_slots.items():
            block = moved(me, axes, other, steps)
            for k, dst in enumerate(outs):
                n = slot * arrays + k
                pltpu.make_async_remote_copy(
                    half(dst, block, 1 - c), half(dst, block, 1 - c),
                    pass_send.at[n], pass_recv.at[n],
                    device_id=(me, 1 - c), device_id_type=MESH,
                ).wait_recv()

    def cost(steps):
        return (sum(1 for s in steps if s), len(steps), [-s for s in steps])

    return [first] + [arrive(steps) for steps in sorted(slots, key=cost)] + [last]


def gather_sems(chips, arrays):
    total = (chips - 1) * arrays
    return [pltpu.SemaphoreType.DMA((total,)) for _ in range(4)] + [
        pltpu.SemaphoreType.DMA((arrays,))
    ]


def gather_kernel(chips, arrays, *refs):
    ins, outs, sems = refs[:arrays], refs[arrays : 2 * arrays], refs[2 * arrays :]
    me, core = lax.axis_index("wide"), lax.axis_index("narrow")
    axes = chip_axes(chips)
    greet(me, core, axes)
    for c in range(2):
        @pl.when(core == c)
        def _():
            for stage in gather_plan(ins, outs, sems, me, c, axes):
                stage()


def gather(arrays, chips, ident):
    vm = pl.BlockSpec(memory_space=pltpu.VMEM)
    return pl.pallas_call(
        functools.partial(gather_kernel, chips, len(arrays)),
        out_shape=[jax.ShapeDtypeStruct((chips,) + a.shape, a.dtype) for a in arrays],
        in_specs=[vm] * len(arrays),
        out_specs=[pl.BlockSpec(memory_space=pl.ANY)] * len(arrays),
        scratch_shapes=gather_sems(chips, len(arrays)),
        compiler_params=pltpu.CompilerParams(collective_id=ident, has_side_effects=True),
    )(*arrays)


def scatter_plan(ins, outs, accs, halves, landed, results, sems, me, c, axes):
    order = axis_orders(axes)[c]
    send, recv, swap_send, swap_recv, own, out_sem, last_send, last_recv = sems
    arrays = len(ins)
    slots = slots_of(axes, order)
    depth = len(order)

    def all_steps(number):
        steps = itertools.product(*grid_of(axes, order[:number]))
        return sorted(steps, key=lambda t: (-sum(1 for s in t if s), [-s for s in reversed(t)]))

    def owner(steps):
        return moved(me, axes, order, steps)

    whole = all_steps(depth)

    def swap(steps, core):
        there = axis_orders(axes)[core]
        names = all_steps_of(there)
        n = names.index(steps)
        block = moved(me, axes, there, steps)
        return [
            pltpu.make_async_remote_copy(
                half(ins[k], block, core), halves[k].at[block],
                swap_send.at[n * arrays + k], swap_recv.at[n * arrays + k],
                device_id=(me, 1 - c), device_id_type=MESH,
            )
            for k in range(arrays)
        ]

    def all_steps_of(there):
        steps = itertools.product(*grid_of(axes, there))
        return sorted(steps, key=lambda t: (-sum(1 for s in t if s), [-s for s in reversed(t)]))

    def load(steps):
        block = owner(steps)
        n = whole.index(steps)
        return [
            pltpu.make_async_copy(half(ins[k], block, c), accs[k].at[block], own.at[n * arrays + k])
            for k in range(arrays)
        ]

    def message(steps):
        block = owner(steps)
        target = moved(me, axes, order[len(steps) - 1 :], steps[-1:])
        slot = slots[steps]
        return [
            pltpu.make_async_remote_copy(
                accs[k].at[block], landed[k].at[slot],
                send.at[slot * arrays + k], recv.at[slot * arrays + k],
                device_id=(target, c), device_id_type=MESH,
            )
            for k in range(arrays)
        ]

    def send_on(steps):
        if steps and steps[-1]:
            for copy in message(steps):
                copy.start()

    def first():
        for steps in all_steps_of(axis_orders(axes)[1 - c]):
            for copy in swap(steps, 1 - c):
                copy.start()
        for steps in whole:
            for copy in load(steps):
                copy.start()

    def add_pair(steps):
        def run():
            for copy in load(steps):
                copy.wait()
            for copy in swap(steps, c):
                copy.wait_recv()
            block = owner(steps)
            for k in range(arrays):
                accs[k][block] = (
                    accs[k][block].astype(F32) + halves[k][block].astype(F32)
                ).astype(BF16)
            send_on(steps)
        return run

    def add(steps):
        def run():
            got = [steps + (s,) for s in range(1, axes[order[len(steps)]][1])]
            for came in got:
                for copy in message(came):
                    copy.wait_recv()
            block = owner(steps)
            for k in range(arrays):
                total = accs[k][block].astype(F32)
                for came in got:
                    total = total + landed[k][slots[came]].astype(F32)
                if steps:
                    accs[k][block] = total.astype(BF16)
                else:
                    width = total.shape[-1]
                    results[k][:, pl.ds(c * width, width)] = total
            if steps:
                send_on(steps)
            else:
                for copy in finals(c):
                    copy.start()
        return run

    def finals(core):
        return [
            pltpu.make_async_remote_copy(
                flat_half(results[k], core), flat_half(results[k], core),
                last_send.at[k], last_recv.at[k],
                device_id=(me, 1 - c), device_id_type=MESH,
            )
            for k in range(arrays)
        ]

    def last():
        for steps in slots:
            for copy in message(steps):
                copy.wait_send()
        for steps in all_steps_of(axis_orders(axes)[1 - c]):
            for copy in swap(steps, 1 - c):
                copy.wait_send()
        outgoing = [pltpu.make_async_copy(results[k], outs[k], out_sem.at[k]) for k in range(arrays)]
        for copy in finals(c):
            copy.wait_send()
        for copy, out in zip(finals(1 - c), outgoing):
            copy.wait_recv()
            out.start()
        for out in outgoing:
            out.wait()

    def settle(steps):
        def run():
            add_pair(steps + (0,))()
            add(steps)()
        return run

    events = [first] + [add_pair(steps) for steps in whole if steps[-1]]
    events += [settle(steps) for steps in all_steps(depth - 1)]
    for number in reversed(range(depth - 1)):
        events += [add(steps) for steps in all_steps(number)]
    return events + [last]


def scatter_scratch(arrays):
    chips = arrays[0].shape[0]
    number = len(arrays)
    scratch = []
    for rows in (chips, chips, chips - 1):
        scratch += [pltpu.VMEM((rows, a.shape[1], a.shape[2] // 2), BF16) for a in arrays]
    scratch += [pltpu.VMEM(a.shape[1:], F32) for a in arrays]
    dma = pltpu.SemaphoreType.DMA
    sizes = (chips - 1,) * 2 + (chips,) * 3 + (1,) * 3
    return scratch + [dma((n * number,)) for n in sizes]


def scatter_parts(arrays, refs):
    parts = [refs[n * arrays : (n + 1) * arrays] for n in range(4)]
    return parts, refs[4 * arrays :]


def scatter_kernel(chips, arrays, *refs):
    ins, outs = refs[:arrays], refs[arrays : 2 * arrays]
    parts, sems = scatter_parts(arrays, refs[2 * arrays :])
    me, core = lax.axis_index("wide"), lax.axis_index("narrow")
    axes = chip_axes(chips)
    greet(me, core, axes)
    for c in range(2):
        @pl.when(core == c)
        def _():
            for stage in scatter_plan(ins, outs, *parts, sems, me, c, axes):
                stage()


def scatter(arrays, ident):
    any_space = pl.BlockSpec(memory_space=pl.ANY)
    return pl.pallas_call(
        functools.partial(scatter_kernel, arrays[0].shape[0], len(arrays)),
        out_shape=[jax.ShapeDtypeStruct(a.shape[1:], F32) for a in arrays],
        in_specs=[any_space] * len(arrays),
        out_specs=[any_space] * len(arrays),
        scratch_shapes=scatter_scratch(arrays),
        compiler_params=pltpu.CompilerParams(
            collective_id=ident, has_side_effects=True, vmem_limit_bytes=60 * 2**20
        ),
    )(*arrays)


def forward_head(qkv, extra, pad, out, lse, head_dim):
    count = qkv.shape[-1]
    factor = head_dim**-0.5 * LOG2E
    keys = jnp.concatenate([qkv[0, head_dim : 2 * head_dim, :], extra[1]], 0).T
    value = qkv[0, 2 * head_dim : 3 * head_dim + SPARE, :]

    for start in range(0, count, CHUNK):
        part = pl.ds(start, CHUNK)
        query = qkv[0, :head_dim, part]
        own_key = qkv[0, head_dim : 2 * head_dim, part]
        own = jnp.sum(query.astype(F32) * own_key.astype(F32), 0, keepdims=True) + pad[:, part]
        raw = dims(keys, jnp.concatenate([query, extra[0, :, part]], 0), 1, 0)
        top = jnp.maximum(jnp.max(raw, 0, keepdims=True), own)
        probs = jnp.exp2((raw - top) * factor).astype(BF16)
        own = jnp.exp2((own - top) * factor)
        both = dims(value, probs, 1, 0)
        total = both[head_dim : head_dim + 1] + own
        own_value = qkv[0, 2 * head_dim : 3 * head_dim, part].astype(F32)
        out[0, :, part] = ((both[:head_dim] + own * own_value) / total).astype(BF16)
        lse[0, :, part] = top + jnp.log2(total) * (1.0 / factor)


def split_rows(row):
    high = row.astype(BF16)
    rest = row - high.astype(F32)
    middle = rest.astype(BF16)
    low = (rest - middle.astype(F32)).astype(BF16)
    return [high, middle, low]


def backward_head(qkv, extra, pad, out, d_out, lse, grad, d_key, d_value, head_dim):
    count = qkv.shape[-1]
    scale = head_dim**-0.5
    factor = scale * LOG2E
    keys = qkv[0, head_dim : 2 * head_dim, :]
    keys_t = jnp.concatenate([keys, extra[1]], 0).T
    row = lax.broadcasted_iota(jnp.int32, (SPARE, count), 0)
    ones = jnp.where(row < 3, 1.0, 0.0).astype(BF16)
    value_t = jnp.concatenate([qkv[0, 2 * head_dim : 3 * head_dim, :], ones], 0).T

    for start in range(0, count, CHUNK):
        part = pl.ds(start, CHUNK)
        query = qkv[0, :head_dim, part]
        d_part = d_out[0, :, part]
        d_full = d_part.astype(F32)
        share = jnp.sum(d_full * out[0, :, part].astype(F32), 0, keepdims=True)
        row = lax.broadcasted_iota(jnp.int32, (SPARE, CHUNK), 0)

        def spread(values, at, base):
            for n, piece in enumerate(split_rows(values)):
                base = jnp.where(row == at + n, -piece.astype(F32), base)
            return base.astype(BF16)

        base = extra[0, :, part].astype(F32)
        query_x = jnp.concatenate([query, spread(lse[0, :, part], 5, base)], 0)
        d_part_x = jnp.concatenate([d_part, spread(share, 0, jnp.zeros_like(base))], 0)
        probs = jnp.exp2(dims(keys_t, query_x, 1, 0) * factor)
        d_scores = (probs * dims(value_t, d_part_x, 1, 0)).astype(BF16)
        probs_low = probs.astype(BF16)

        own_key = qkv[0, head_dim : 2 * head_dim, part].astype(F32)
        own_value = qkv[0, 2 * head_dim : 3 * head_dim, part].astype(F32)
        query_f = query.astype(F32)
        own = jnp.sum(query_f * own_key, 0, keepdims=True) + pad[:, part]
        own = jnp.exp2((own - lse[0, :, part]) * factor)
        own_ds = own * (jnp.sum(d_full * own_value, 0, keepdims=True) - share)

        grad[0, :head_dim, part] = (
            (dims(keys, d_scores, 1, 0) + own_ds * own_key) * scale
        ).astype(BF16)
        more_value = dims(d_part, probs_low, 1, 1)
        more_key = dims(query, d_scores, 1, 1)
        if start == 0:
            d_value[...] = more_value
            d_key[...] = more_key
        else:
            d_value[...] += more_value
            d_key[...] += more_key
        grad[0, head_dim : 2 * head_dim, part] = (own_ds * query_f).astype(BF16)
        grad[0, 2 * head_dim : 3 * head_dim, part] = (own * d_full).astype(BF16)
    for slot, total, factor_out in ((1, d_key, scale), (2, d_value, 1.0)):
        rows = pl.ds(slot * head_dim, head_dim)
        whole = total[...]
        grad[0, rows, :] = ((whole + grad[0, rows, :].astype(F32)) * factor_out).astype(BF16)
    grad[0, 3 * head_dim :, :] = jnp.zeros((SPARE, count), BF16)


def head_spec(rows, count):
    return pl.BlockSpec((1, rows, count), lambda h: (h, 0, 0))


def same(*shape):
    return pl.BlockSpec(shape, lambda h: (0,) * len(shape))


def gather_step(n, count):
    return 4 + n * 22 // count


def scatter_step(n, count):
    return n // 2 if n < 8 else n - 4


def spread_over(number, when):
    inner = number - 2
    steps = [when(n, inner) for n in range(inner)]
    return [0] + [min(step, HEADS - 1) for step in steps] + [HEADS - 1]


def run_stages(plan, when, chips):
    me, core = lax.axis_index("wide"), lax.axis_index("narrow")
    axes = chip_axes(chips)
    h = pl.program_id(0)

    @pl.when(h == 0)
    def _():
        greet(me, core, axes)

    for c in range(2):
        stages = plan(me, c, axes)
        for stage, step in zip(stages, spread_over(len(stages), when)):
            @pl.when((core == c) & (h == step))
            def _(stage=stage):
                stage()


def attention(qkv, extra, pad, weights=(), chips=0, ident=None):
    rows, count = qkv.shape[1:]
    head_dim = (rows - SPARE) // 3
    n = len(weights)

    def body(*refs):
        (qkv_ref, extra_ref, pad_ref), ins = refs[:3], refs[3 : 3 + n]
        (out, lse), outs, sems = refs[3 + n : 5 + n], refs[5 + n : 5 + 2 * n], refs[5 + 2 * n :]
        if n:
            run_stages(
                lambda me, c, axes: gather_plan(ins, outs, sems, me, c, axes),
                gather_step, chips,
            )
        forward_head(qkv_ref, extra_ref, pad_ref, out, lse, head_dim)

    return pl.pallas_call(
        body,
        grid=(HEADS,),
        out_shape=[
            jax.ShapeDtypeStruct((HEADS, head_dim, count), BF16),
            jax.ShapeDtypeStruct((HEADS, 1, count), F32),
        ]
        + [jax.ShapeDtypeStruct((chips,) + a.shape, a.dtype) for a in weights],
        in_specs=[head_spec(rows, count), same(2, SPARE, count), same(1, count)]
        + [same(*a.shape) for a in weights],
        out_specs=[head_spec(head_dim, count), head_spec(1, count)]
        + [pl.BlockSpec(memory_space=pl.ANY)] * n,
        scratch_shapes=gather_sems(chips, n) if n else [],
        compiler_params=pltpu.CompilerParams(
            vmem_limit_bytes=60 * 2**20, collective_id=ident, has_side_effects=n > 0
        ),
    )(qkv, extra, pad, *weights)


def attention_back(qkv, extra, pad, out, d_out, lse, grads=(), chips=0, ident=None):
    rows, count = qkv.shape[1:]
    head_dim = (rows - SPARE) // 3
    n = len(grads)

    def body(*refs):
        ins, refs = refs[:6], refs[6:]
        g_ins, grad, g_outs, rest = refs[:n], refs[n], refs[n + 1 : 2 * n + 1], refs[2 * n + 1 :]
        d_key, d_value = rest[:2]
        if n:
            parts, sems = scatter_parts(n, rest[2:])
            run_stages(
                lambda me, c, axes: scatter_plan(g_ins, g_outs, *parts, sems, me, c, axes),
                scatter_step, chips,
            )
        backward_head(*ins, grad, d_key, d_value, head_dim)

    any_space = pl.BlockSpec(memory_space=pl.ANY)
    return pl.pallas_call(
        body,
        grid=(HEADS,),
        out_shape=[jax.ShapeDtypeStruct((HEADS, rows, count), BF16)]
        + [jax.ShapeDtypeStruct(a.shape[1:], F32) for a in grads],
        in_specs=[
            head_spec(rows, count),
            same(2, SPARE, count),
            same(1, count),
            head_spec(head_dim, count),
            head_spec(head_dim, count),
            head_spec(1, count),
        ]
        + [any_space] * n,
        out_specs=[head_spec(rows, count)] + [any_space] * n,
        scratch_shapes=[pltpu.VMEM((head_dim, count), F32)] * 2
        + (scatter_scratch(grads) if n else []),
        compiler_params=pltpu.CompilerParams(
            vmem_limit_bytes=60 * 2**20, collective_id=ident, has_side_effects=n > 0
        ),
    )(qkv, extra, pad, out, d_out, lse, *grads)


def masking_rows(seg, live):
    n = jnp.arange(SPARE)[:, None]
    seg, live = seg[None], live[None]
    group = n < SEGS
    query = jnp.where(group, seg == n, n == SEGS).astype(F32)
    keys = jnp.where(
        group,
        jnp.where(seg == n, 0.0, MASKED),
        jnp.where(
            n == SEGS,
            jnp.where(live > 0, 0.0, MASKED),
            jnp.where((n > SEGS) & (n < SEGS + 4), 1.0, 0.0),
        ),
    )
    return jnp.stack([query, keys]).astype(BF16), jnp.where(live > 0, MASKED, 0.0).astype(F32)


def norm(values):
    centred = values - jnp.mean(values, -1, keepdims=True)
    factor = lax.rsqrt(jnp.mean(centred * centred, -1, keepdims=True) + 1e-05)
    return centred * factor, factor


def norm_back(grad, normed, factor, gain):
    scaled = grad * gain
    inner = (
        scaled
        - jnp.mean(scaled, -1, keepdims=True)
        - normed * jnp.mean(scaled * normed, -1, keepdims=True)
    )
    return factor * inner, jnp.sum(grad * normed, 0), jnp.sum(grad, 0)


def gelu_pair(values):
    cdf = 0.5 * (1.0 + lax.erf(values * (1.0 / math.sqrt(2.0))))
    pdf = jnp.exp(-0.5 * values * values) * (1.0 / math.sqrt(2.0 * math.pi))
    return values * cdf, cdf + values * pdf


def by_rows(values):
    return with_layout_constraint(values, Layout((0, 1)))


def row_sums(values):
    return dims(jnp.ones((8, values.shape[0]), BF16), values, 1, 0)[0]


def widen(vector, width):
    return jnp.pad(vector, (0, width - vector.shape[0]))


def shards(
    chips,
    replicas,
    tokens,
    segment,
    keep,
    cotangent,
    gain_one,
    bias_one,
    w_query,
    b_query,
    w_key,
    w_value,
    b_value,
    w_out,
    b_out,
    gain_two,
    bias_two,
    w_hidden,
    b_hidden,
    w_proj,
    b_proj,
):
    own_copies = chips == HEADS and replicas == 2
    count, width = tokens.shape
    head_dim = width // HEADS
    hidden = w_hidden.shape[1] * chips
    vectors = (gain_one, bias_one, b_query, b_value, b_out, gain_two, bias_two, b_hidden, b_proj)
    packed = widen(jnp.concatenate(vectors), width)[None]
    packed = jnp.pad(packed, ((0, SPARE - 1), (0, 0)))
    ends = list(itertools.accumulate(v.shape[0] for v in vectors))

    if own_copies:
        first = jnp.concatenate([w_query.T, w_key.T, w_value.T, packed], 0)
        (first,) = gather([first], chips, 0)
        joined_t = first
        vector_rows = first[:, 3 * head_dim :, :]
    else:
        whole = [
            lax.all_gather(w.T, "wide", axis=0, tiled=True) for w in (w_query, w_key, w_value)
        ]
        whole = [w.reshape(HEADS, head_dim, width) for w in whole]
        whole.append(jnp.zeros((HEADS, SPARE, width), BF16))
        joined_t = jnp.concatenate(whole, 1)
        vector_rows = lax.all_gather(packed, "wide", axis=0, tiled=False)
        out_t, hidden_t, proj_t = [
            lax.all_gather(w.T, "wide", axis=0, tiled=False) for w in (w_out, w_hidden, w_proj)
        ]
    joined_t = joined_t.reshape(HEADS * (3 * head_dim + SPARE), width)
    gain_one_f, bias_one_f, b_query_f, b_value_f, b_out_f, gain_two_f, bias_two_f, b_hidden_f, b_proj_f = [
        vector_rows[:, 0, end - v.shape[0] : end].reshape(-1).astype(F32)
        for v, end in zip(vectors, ends)
    ]

    live = keep[0]
    seg = segment[0]
    extra, pad = masking_rows(seg, live)

    x = by_rows(tokens).astype(F32)
    xhat_one, factor_one = norm(x)
    h_one = lax.optimization_barrier((xhat_one * gain_one_f + bias_one_f).astype(BF16))
    block = 3 * head_dim + SPARE
    offsets = jnp.concatenate(
        [
            b_query_f.reshape(HEADS, head_dim),
            jnp.zeros((HEADS, head_dim), F32),
            b_value_f.reshape(HEADS, head_dim),
            jnp.zeros((HEADS, SPARE), F32),
        ],
        1,
    )
    row = jnp.arange(block)[None, :, None]
    qkv = dims(joined_t, h_one, 1, 1).reshape(HEADS, block, count) + offsets[:, :, None]
    qkv = jnp.where(row < 3 * head_dim, qkv, jnp.where(row == 3 * head_dim, 1.0, 0.0)).astype(BF16)
    if own_copies:
        o_t, lse, out_t, hidden_t, proj_t = attention(
            qkv, extra, pad, (w_out.T, w_hidden.T, w_proj.T), chips, 1
        )
    else:
        o_t, lse = attention(qkv, extra, pad)
    out_t = out_t.reshape(width, width)
    hidden_t = hidden_t.reshape(hidden, width)
    proj_t = proj_t.reshape(width, hidden)
    o_flat = o_t.reshape(width, count)
    x_one = by_rows(x + dims(o_flat, out_t, 0, 1) + b_out_f)
    xhat_two, factor_two = norm(x_one)
    h_two = lax.optimization_barrier((xhat_two * gain_two_f + bias_two_f).astype(BF16))
    upper = dims(h_two, hidden_t, 1, 1) + b_hidden_f
    act, slope = lax.optimization_barrier([v.astype(BF16) for v in gelu_pair(upper)])
    mixed = (x_one + dims(act, proj_t, 1, 1) + b_proj_f).astype(BF16)

    d_y = by_rows(cotangent).astype(F32) * live.astype(F32)[:, None]
    d_m = d_y.astype(BF16)
    grad_proj = dims(d_m, act, 0, 0).astype(BF16)
    d_upper = (dims(d_m, proj_t, 1, 0) * slope.astype(F32)).astype(BF16)
    grad_hidden = dims(d_upper, h_two, 0, 0).astype(BF16)
    d_two, grad_gain_two, grad_bias_two = norm_back(
        dims(d_upper, hidden_t, 1, 0), xhat_two, factor_two, gain_two_f
    )
    d_x_one = by_rows(d_y + d_two)
    d_attn = d_x_one.astype(BF16)
    grad_out = dims(d_attn, o_flat, 0, 1).astype(BF16)
    d_o = dims(out_t, d_attn, 0, 1).astype(BF16).reshape(HEADS, head_dim, count)
    late = [
        g.reshape(chips, -1, g.shape[-1]) for g in (grad_out, grad_hidden, grad_proj)
    ]
    if own_copies:
        d_qkv, *late = attention_back(qkv, extra, pad, o_t, d_o, lse, late, chips, 2)
    else:
        (d_qkv,) = attention_back(qkv, extra, pad, o_t, d_o, lse)
    d_flat = d_qkv.reshape(HEADS * block, count)
    grad_qkv = dims(d_flat, h_one, 1, 0).reshape(HEADS, block, width)
    bias_sums = dims(jnp.ones((8, count), BF16), d_flat, 1, 1)[0].reshape(HEADS, block)
    d_one, grad_gain_one, grad_bias_one = norm_back(
        dims(d_flat, joined_t, 0, 0), xhat_one, factor_one, gain_one_f
    )
    grad_tokens = d_x_one + d_one

    part = width // chips
    sums = jnp.stack([
        grad_gain_one,
        grad_bias_one,
        bias_sums[:, :head_dim].reshape(-1),
        bias_sums[:, 2 * head_dim : 3 * head_dim].reshape(-1),
        row_sums(d_attn),
        grad_gain_two,
        grad_bias_two,
        row_sums(d_m),
    ])
    sums = sums.reshape(-1, chips, part).transpose(1, 0, 2)
    more = row_sums(d_upper).reshape(chips, -1, part)
    sums = jnp.concatenate([sums, more], 1)
    sums = jnp.pad(sums, ((0, 0), (0, SPARE - sums.shape[1]), (0, width - part)))
    if own_copies:
        early = jnp.concatenate([grad_qkv[:, : 3 * head_dim], sums], 1).astype(BF16)
        (early,) = scatter([early], 3)
        grads = [early[n * head_dim : (n + 1) * head_dim] for n in range(3)]
        vector_grads = early[3 * head_dim :]
    else:
        grads = [
            grad_qkv[:, n * head_dim : (n + 1) * head_dim].reshape(chips, part, width)
            for n in range(3)
        ]
        *grads, vector_grads = [
            lax.psum(
                lax.psum_scatter(g.astype(F32), "wide", scatter_dimension=0, tiled=False).astype(
                    BF16
                ),
                "narrow",
            ).astype(F32)
            for g in grads + [sums]
        ]
        late = [
            lax.psum(
                lax.psum_scatter(g.astype(F32), "wide", scatter_dimension=0, tiled=False).astype(
                    BF16
                ),
                "narrow",
            ).astype(F32)
            for g in late
        ]
    g_query, g_key, g_value = [g.T for g in grads]
    g_out, g_hidden, g_proj = [g.T for g in late]
    g_vec = [vector_grads[n, :part] for n in range(8)]
    ratio = hidden // width
    g_vec.insert(7, vector_grads[8 : 8 + ratio, :part].reshape(-1))
    return (
        mixed, grad_tokens, g_vec[0], g_vec[1], g_query, g_vec[2], g_key, g_value, g_vec[3],
        g_out, g_vec[4], g_vec[5], g_vec[6], g_hidden, g_vec[7], g_proj, g_vec[8],
    )


def solution(mesh):
    both, wide = P(("wide", "narrow"), None), P("wide")
    weight = P(None, "wide")
    return jax.shard_map(
        functools.partial(shards, mesh.shape["wide"], mesh.shape["narrow"]),
        mesh=mesh,
        in_specs=(
            both, both, both, both, wide, wide, weight, wide, weight, weight, wide, weight, wide,
            wide, wide, weight, wide, weight, wide,
        ),
        out_specs=(
            both, both, wide, wide, weight, wide, weight, weight, wide, weight, wide, wide, wide,
            weight, wide, weight, wide,
        ),
        check_vma=False,
    )
```
